32 devices in a mesh: grid: 8 (over z, y), dom: 4 (over x, core).
Axes of the slice: x: 2, y: 2, z: 4, core: 2. Of those that a mesh axis runs over, the one named last changes fastest.
Arguments:
- fields: float32 [8, 16, 16, 16, 256], P('grid', 'dom'), may hold values from -6 to 6
- cutoffs: int32 [8, 4], P('grid'), may hold values from 0 to 2
- weights: int32 [8], P('grid'), may hold values from -3 to 3, as said below
- diffusion: float32 [4], replicated, may hold values from 0.03 to 0.12
- courant: float32 [4], replicated, may hold values from -0.2 to 0.2
Outputs:
- combined_fields: float32 [8, 16, 16, 16, 256], P('grid', 'dom')
The draws below stay inside these ranges and needn't reach their ends.
Inputs may be any that keep to these rules, and one draw needn't show every extreme that they name: `weights`: each weight is a nonzero integer of magnitude 1 to 3.
All inputs are finite; a program needn't handle non-finite values.
Results may differ from the reference program's by a relative error of at most 0.0003.
Values sent between devices are 32-bit elements; how exact they have to be, the bound alone decides.
No kernel may reach another device: no remote copies, remote signals or barrier semaphores. Data moves between devices by JAX's collectives and lax.ppermute only.
A program may use at most 64 MiB of HBM per device.

```python
import jax
import jax.numpy as jnp
from jax import lax

N2 = 16
N3 = 16
N4 = 256
STEPS = 2
N1 = 16
GRIDS = 8


def draw_weights(key, part):
    magnitude = jax.random.randint(jax.random.fold_in(key, 11), (GRIDS,), 1, 4, dtype=jnp.int32)
    sign_bits = jax.random.randint(jax.random.fold_in(key, 23), (GRIDS,), 0, 2, dtype=jnp.int32)
    return magnitude * (2 * sign_bits - 1)


def place_ends(entries, rng, least, largest):
    dims = entries.shape
    place = [jax.random.randint(jax.random.fold_in(rng, axis), (), 0, dims[axis]) for axis in range(len(dims))]
    entries = entries.at[tuple(place)].set(least)
    longest = dims.index(max(dims))
    place[longest] = (place[longest] + 1) % dims[longest]
    return entries.at[tuple(place)].set(largest)


def shard_levels(stream_key, shape, pieces, smallest, top_value):
    level = 1.0
    for dim, shards_of in pieces:
        draws = jax.random.uniform(jax.random.fold_in(jax.random.fold_in(stream_key, 6), dim), (shards_of,), jnp.float32, smallest / len(pieces), top_value / len(pieces))
        level = level * jnp.repeat(jnp.exp(draws), shape[dim] // shards_of).reshape((-1,) + (1,) * (len(shape) - 1 - dim))
    return level


def centred(own_key, extent, spread, most, shards=(), kind=jnp.bfloat16):
    level = shard_levels(own_key, extent, shards, -0.22, 0.18) if shards else 1.0
    values = jax.random.normal(own_key, extent, jnp.float32) * spread * level
    return jnp.minimum(jnp.maximum(values, -most), most).astype(kind)


def setup_inputs(seed: int = 0) -> dict:
    arg_keys = jax.random.split(jax.random.key(seed), 6)
    fields = centred(arg_keys[0], (GRIDS, N1, N2, N3, N4), 1.0, 6.0, ((0, 8), (1, 4)), jnp.float32)
    cutoffs = place_ends(jax.random.randint(arg_keys[1], (GRIDS, 4), 0, 3), jax.random.fold_in(arg_keys[1], 1), 0, 2).astype(jnp.int32)
    weights = draw_weights(jax.random.fold_in(arg_keys[5], 71), 0)
    diffusion = jnp.clip(jax.random.uniform(arg_keys[3], (4,), jnp.float32, 0.03, 0.12), 0.03, 0.12)
    courant = jnp.clip(jax.random.uniform(arg_keys[4], (4,), jnp.float32, -0.2, 0.2), -0.2, 0.2)
    return {"fields": fields, "cutoffs": cutoffs, "weights": weights, "diffusion": diffusion, "courant": courant}


def neighbours(length):
    positions = jnp.arange(length, dtype=jnp.int32)
    spacing = jnp.bitwise_and(positions, -positions)
    left_at = jnp.remainder(positions - spacing, length).astype(jnp.int32)
    right_at = jnp.remainder(positions + spacing, length).astype(jnp.int32)
    return positions, spacing, left_at, right_at


def shaped(vector, axis_at, order_of):
    dims_list = [1] * order_of
    dims_list[axis_at] = vector.shape[0]
    return vector.reshape(dims_list)


def hierarchize(values, axis_at):
    length = values.shape[axis_at]
    positions, spacing, left_at, right_at = neighbours(length)
    factor = shaped(jnp.where(positions > 0, 0.5, 0.0).astype(jnp.float32), axis_at, values.ndim)
    return values - factor * (jnp.take(values, left_at, axis=axis_at) + jnp.take(values, right_at, axis=axis_at))


def dehierarchize(values, axis_at):
    length = values.shape[axis_at]
    positions, spacing, left_at, right_at = neighbours(length)
    for level_bit in reversed(range(length.bit_length() - 1)):
        factor = shaped(jnp.where(spacing == 2 ** level_bit, 0.5, 0.0).astype(jnp.float32), axis_at, values.ndim)
        values = values + factor * (jnp.take(values, left_at, axis=axis_at) + jnp.take(values, right_at, axis=axis_at))
    return values


def tendency(centre, neighbour_pairs, diffusion, courant):
    result = jnp.zeros_like(centre)
    for axis_at in range(4):
        forward, behind = neighbour_pairs[axis_at]
        result = result + diffusion[axis_at] * (forward - 2.0 * centre + behind) - courant[axis_at] * (forward - behind)
    return result


def rate_full(values, diffusion, courant):
    neighbour_pairs = [(jnp.roll(values, -1, axis_at), jnp.roll(values, 1, axis_at)) for axis_at in range(4)]
    return tendency(values, neighbour_pairs, diffusion, courant)


def kept_mask(cutoff_row, position_lists):
    kept_cells = jnp.ones((1, 1, 1, 1), jnp.float32)
    for axis_at in range(4):
        stride = jnp.left_shift(jnp.int32(1), cutoff_row[axis_at].astype(jnp.int32))
        divides = (jnp.remainder(position_lists[axis_at], stride) == 0).astype(jnp.float32)
        kept_cells = kept_cells * shaped(divides, axis_at, 4)
    return kept_cells


def reference(fields, cutoffs, weights, diffusion, courant):
    grid_shape = fields.shape[1:]
    position_lists = [jnp.arange(grid_shape[axis_at], dtype=jnp.int32) for axis_at in range(4)]

    def accumulate(running, operand):
        solution, cutoff_row, weight = operand
        for stepping in range(STEPS):
            section_one = solution + rate_full(solution, diffusion, courant)
            section_two = 0.75 * solution + 0.25 * (section_one + rate_full(section_one, diffusion, courant))
            solution = solution / 3.0 + (2.0 / 3.0) * (section_two + rate_full(section_two, diffusion, courant))
        for axis_at in range(4):
            solution = hierarchize(solution, axis_at)
        term = weight.astype(jnp.float32) * kept_mask(cutoff_row, position_lists) * solution
        return running + term, None

    summed, unused = lax.scan(accumulate, jnp.zeros(grid_shape, jnp.float32), (fields, cutoffs, weights))
    summed = summed / GRIDS

    def restore(cutoff_row):
        values = kept_mask(cutoff_row, position_lists) * summed
        for axis_at in range(4):
            values = dehierarchize(values, axis_at)
        return values

    return lax.map(restore, cutoffs)
```

```python
import functools

import jax
import jax.numpy as jnp
from jax import lax
from jax.experimental import pallas as pl
from jax.experimental.pallas import tpu as pltpu
from jax.sharding import PartitionSpec as P

STEPS = 2
HALO = 8
TILE = 8

VMEM = pl.BlockSpec(memory_space=pltpu.VMEM)
SMEM = pl.BlockSpec(memory_space=pltpu.SMEM)


def swap_pairs(size, bit):
    return [(i, i ^ bit) for i in range(size)]


def swapped(x, axis, bit):
    return lax.ppermute(x, axis, swap_pairs(lax.axis_size(axis), bit))


def split_product(x, m_high, m_low=None, dims=(((1,), (0,)), ((), ()))):
    high = x.astype(jnp.bfloat16)
    low = (x - high.astype(jnp.float32)).astype(jnp.bfloat16)
    dot = functools.partial(lax.dot_general, dimension_numbers=dims, preferred_element_type=jnp.float32)
    total = dot(high, m_high) + dot(low, m_high)
    return total if m_low is None else total + dot(high, m_low)


def lane_places(second_len, third_len):
    shape = (second_len * third_len,) * 2
    row, col = (lax.broadcasted_iota(jnp.int32, shape, d) for d in (0, 1))
    return (row // third_len, col // third_len, second_len), (row % third_len, col % third_len, third_len)


def rate_matrix(second_len, third_len, diffusion, courant):
    (s_row, s_col, s_len), (t_row, t_col, t_len) = lane_places(second_len, third_len)

    def hop(row, col, length, by):
        return row == jnp.remainder(col + by, length)

    def where(cond, value):
        return jnp.where(cond, value, 0.0)

    same_s, same_t = s_row == s_col, t_row == t_col
    return (
        where(same_s & same_t, -2.0 * jnp.sum(diffusion))
        + where(hop(s_row, s_col, s_len, 1) & same_t, diffusion[1] - courant[1])
        + where(hop(s_row, s_col, s_len, -1) & same_t, diffusion[1] + courant[1])
        + where(hop(t_row, t_col, t_len, 1) & same_s, diffusion[2] - courant[2])
        + where(hop(t_row, t_col, t_len, -1) & same_s, diffusion[2] + courant[2])
    )


def surplus_entry(source, target, length):
    hop = jnp.where(target % 4 == 0, 0, jnp.where(target % 2 == 0, 2, 1))
    beside = (source == (target + hop) % length).astype(jnp.float32) + (source == (target - hop) % length).astype(
        jnp.float32
    )
    return (source == target).astype(jnp.float32) - jnp.where(hop > 0, 0.5, 0.0) * beside


def restore_entry(source, target, length):
    def at(by):
        return (source == (target + by) % length).astype(jnp.float32)

    lower, upper = (at(-1), at(1))
    inner = jnp.where(
        target % 4 == 1,
        0.75 * lower + 0.5 * upper + 0.25 * at(3),
        0.75 * upper + 0.5 * lower + 0.25 * at(-3),
    )
    beside = jnp.where(target % 4 == 0, 0.0, jnp.where(target % 4 == 2, 0.5 * (at(-2) + at(2)), inner))
    return at(0) + beside


def divides(place, cutoff):
    return (jnp.bitwise_and(place, jnp.left_shift(1, cutoff) - 1) == 0).astype(jnp.float32)


def windows_kernel(dom, u_ref, *refs):
    out_refs, ext = refs[:-1], refs[-1]
    rows, _, length = u_ref.shape
    block = length // dom
    width = block + 2 * HALO
    place = lax.axis_index("dom")
    for r in range(rows):
        turned = u_ref[r].T
        ext[pl.ds(HALO, length), :] = turned
        ext[pl.ds(0, HALO), :] = turned[length - HALO :]
        ext[pl.ds(HALO + length, HALO), :] = turned[:HALO]
        for k in range(dom):
            start = pl.multiple_of((place ^ k) * block, TILE)
            out_refs[k][r] = ext[pl.ds(start, width), :]


def windows(u, dom):
    rows, lanes, length = u.shape
    width = length // dom + 2 * HALO
    return pl.pallas_call(
        functools.partial(windows_kernel, dom),
        out_shape=[jax.ShapeDtypeStruct((rows, width, lanes), jnp.float32)] * dom,
        in_specs=[VMEM],
        out_specs=[VMEM] * dom,
        scratch_shapes=[pltpu.VMEM((length + 2 * HALO, lanes), jnp.float32)],
    )(u)


def evolve_kernel(plan, cut_ref, diff_ref, cour_ref, rate_high, rate_low, lane_surplus, *refs):
    dom, pieces, chain_orders, chunk = plan
    in_refs, refs = refs[:dom], refs[dom:]
    out_refs, (u, w1, w2) = refs[:-3], refs[-3:]
    rows = in_refs[0].shape[0]
    total, width, lanes = u.shape
    block = width - 2 * HALO
    place = lax.axis_index("dom")
    own = lax.axis_index("grid") & (pieces - 1)
    for k in range(dom):
        u[pl.ds((place ^ k) * rows, rows)] = in_refs[k][...]

    def stage(source, target, which, part):
        first = [part * (diff_ref[d] - cour_ref[d]) for d in (0, 3)]
        second = [part * (diff_ref[d] + cour_ref[d]) for d in (0, 3)]

        def body(c, carry):
            start = c * chunk
            here = [source[start + r] for r in range(chunk)]
            before = source[lax.rem(start + total - 1, total)]
            after = source[lax.rem(start + chunk, total)]
            flat = jnp.concatenate(here, axis=0)
            product = split_product(flat, rate_high[which], rate_low[which])
            for r in range(chunk):
                below = here[r - 1] if r else before
                above = here[r + 1] if r + 1 < chunk else after
                target[start + r] = (
                    u[start + r]
                    + product[r * width : (r + 1) * width]
                    + (first[0] * above + second[0] * below)
                    + (first[1] * pltpu.roll(here[r], width - 1, 0) + second[1] * pltpu.roll(here[r], 1, 0))
                )
            return carry

        lax.fori_loop(0, total // chunk, body, 0)

    for _ in range(STEPS):
        stage(u, w1, 0, 1.0 / 3.0)
        stage(w1, w2, 1, 0.5)
        stage(w2, u, 2, 1.0)

    cell = lax.broadcasted_iota(jnp.int32, (block, lanes), 0)
    kept = divides(cell, cut_ref[0, 3])
    odd, twice = cell % 2 == 1, cell % 4 == 2
    near = jnp.where(odd, -0.5, 0.0) * kept
    far = jnp.where(twice, -0.5, 0.0) * kept

    def lines(c, carry):
        start = c * chunk
        flat = jnp.concatenate([u[start + r] for r in range(chunk)], axis=0)
        product = split_product(flat, lane_surplus[...])
        for r in range(chunk):
            v = product[r * width : (r + 1) * width]

            def at(by):
                return pltpu.roll(v, (width - HALO - by) % width, 0)[:block]

            w1[start + r, pl.ds(0, block), :] = kept * at(0) + near * (at(1) + at(-1)) + far * (at(2) + at(-2))
        return carry

    lax.fori_loop(0, total // chunk, lines, 0)

    depth = block // pieces
    half = total // len(chain_orders)
    for chain, order in enumerate(chain_orders):
        keep_ref, send_ref = out_refs[2 * chain], out_refs[2 * chain + 1]
        for slot, q in enumerate(order):
            offset = pl.multiple_of((own ^ q) * depth, TILE)
            out, index = (keep_ref, slot) if slot < len(order) // 2 else (send_ref, slot - len(order) // 2)

            def row(i):
                return w1[i % total, pl.ds(offset, depth), :]

            for r in range(half):
                i = chain * half + r
                if i % 4 == 0:
                    out[index, r] = row(i)
                else:
                    hop = 2 if i % 2 == 0 else 1
                    scale = divides(jnp.int32(i), cut_ref[0, 0])
                    out[index, r] = scale * (row(i) - 0.5 * (row(i - hop) + row(i + hop)))


def evolve(cutoffs, diffusion, courant, rate_parts, lane_surplus, parts, pieces, chain_orders):
    dom = len(parts)
    rows, width, lanes = parts[0].shape
    total = rows * dom
    depth = (width - 2 * HALO) // pieces
    piece = (pieces // 2, total // len(chain_orders), depth, lanes)
    chunk = 4
    return pl.pallas_call(
        functools.partial(evolve_kernel, (dom, pieces, chain_orders, chunk)),
        out_shape=[jax.ShapeDtypeStruct(piece, jnp.float32)] * (2 * len(chain_orders)),
        in_specs=[SMEM] * 3 + [VMEM] * (3 + dom),
        out_specs=[VMEM] * (2 * len(chain_orders)),
        scratch_shapes=[pltpu.VMEM((total, width, lanes), jnp.float32)] * 3,
    )(cutoffs, diffusion, courant, *rate_parts, lane_surplus, *parts)


def rows_kernel(dom, scale, *refs):
    chains = (len(refs) - dom) // 2
    out_refs = refs[2 * chains :]
    half = refs[0].shape[0]
    total = half * chains
    rows = total // dom
    place = lax.axis_index("dom")
    summed = [(refs[2 * c][...] + refs[2 * c + 1][...]) * scale for c in range(chains)]

    def body(all_rows):
        for c in range(chains):
            all_rows[pl.ds(c * half, half)] = summed[c]
        all_rows[pl.ds(total, 1)] = summed[0][:1]
        for k in range(dom):
            out_refs[k][...] = all_rows[pl.ds((place ^ k) * rows, rows + 1)]

    pl.run_scoped(body, pltpu.VMEM((total + 1, *refs[0].shape[1:]), jnp.float32))


def rows_for(dom, scale, ends):
    half, depth, lanes = ends[0].shape
    rows = half * len(ends) // 2 // dom
    return pl.pallas_call(
        functools.partial(rows_kernel, dom, scale),
        out_shape=[jax.ShapeDtypeStruct((rows + 1, depth, lanes), jnp.float32)] * dom,
        in_specs=[VMEM] * len(ends),
        out_specs=[VMEM] * dom,
    )(*ends)


def restore_kernel(plan, cut_ref, lane_restore, *refs):
    dom, pieces, groups = plan
    in_refs, out_ref, summed = refs[:-2], refs[-2], refs[-1]
    rows, lanes, length = out_ref.shape
    place = lax.axis_index("dom")
    own = lax.axis_index("grid") & (pieces - 1)
    depth = length // (dom * pieces)
    for ref, (slots, ks) in zip(in_refs, groups):
        for s, q in enumerate(slots):
            for m, k in enumerate(ks):
                at = pl.multiple_of(((place ^ k) * pieces + (own ^ q)) * depth, TILE)
                summed[:, pl.ds(at, depth), :] = ref[s, m]

    cell = lax.broadcasted_iota(jnp.int32, (length, lanes), 0)
    kept = divides(cell, cut_ref[0, 3])
    odd, twice = cell % 2 == 1, cell % 4 == 2
    far = jnp.where(twice, 0.5, 0.0)
    near = jnp.where(odd, 0.5, 0.0)

    def along_cells(v):
        v = kept * v
        v = v + far * (pltpu.roll(v, length - 2, 0) + pltpu.roll(v, 2, 0))
        v = v + near * (pltpu.roll(v, length - 1, 0) + pltpu.roll(v, 1, 0))
        high = v.astype(jnp.bfloat16)
        low = (v - high.astype(jnp.float32)).astype(jnp.bfloat16)
        dims = (((1,), (1,)), ((), ()))
        dot = functools.partial(lax.dot_general, dimension_numbers=dims, preferred_element_type=jnp.float32)
        return dot(lane_restore[...], high) + dot(lane_restore[...], low)

    one = divides(jnp.int32(1), cut_ref[0, 0])
    two = divides(jnp.int32(2), cut_ref[0, 0])
    for r in range(0, rows, 4):
        first, last = summed[r], summed[r + 4]
        middle = two * summed[r + 2] + 0.5 * (first + last)
        out_ref[r] = along_cells(first)
        out_ref[r + 1] = along_cells(one * summed[r + 1] + 0.5 * (first + middle))
        out_ref[r + 2] = along_cells(middle)
        out_ref[r + 3] = along_cells(one * summed[r + 3] + 0.5 * (middle + last))


def restore(cutoffs, lane_restore, arrays, groups, dom, pieces, rows, lanes, length):
    return pl.pallas_call(
        functools.partial(restore_kernel, (dom, pieces, groups)),
        out_shape=jax.ShapeDtypeStruct((rows, lanes, length), jnp.float32),
        in_specs=[SMEM, VMEM] + [VMEM] * len(arrays),
        out_specs=VMEM,
        scratch_shapes=[pltpu.VMEM((rows + 1, length, lanes), jnp.float32)],
    )(cutoffs, lane_restore, *arrays)


def slot_order(bits):
    order = [0]
    for bit in reversed(bits):
        order = order + [q | bit for q in order]
    return order


def shards(fields, cutoffs, weights, diffusion, courant):
    rows, second_len, third_len, length = fields.shape[1:]
    lanes = second_len * third_len
    dom, grids = lax.axis_size("dom"), lax.axis_size("grid")
    block = length // dom
    pieces = min(grids, block // TILE)
    bits = [1 << i for i in range(grids.bit_length() - 1)]
    halving = [b for b in bits if b < pieces]
    doubling = [b for b in bits if b >= pieces]
    chain_bits = [halving, halving[1:] + halving[:1]]
    chain_orders = tuple(tuple(slot_order(b)) for b in chain_bits)

    base = rate_matrix(second_len, third_len, diffusion, courant)
    rate = jnp.stack([base / 3.0, base * 0.5, base])
    rounded = lax.reduce_precision(rate, exponent_bits=8, mantissa_bits=7)
    rate_high, rate_low = rounded.astype(jnp.bfloat16), (rate - rounded).astype(jnp.bfloat16)
    (s_row, s_col, s_len), (t_row, t_col, t_len) = lane_places(second_len, third_len)
    cut = cutoffs[0]
    lane_surplus = (
        surplus_entry(s_row, s_col, s_len)
        * surplus_entry(t_row, t_col, t_len)
        * (divides(s_col, cut[1]) * divides(t_col, cut[2]))
        * weights[0].astype(jnp.float32)
    ).astype(jnp.bfloat16)
    lane_restore = (
        restore_entry(s_col, s_row, s_len)
        * restore_entry(t_col, t_row, t_len)
        * (divides(s_col, cut[1]) * divides(t_col, cut[2]))
    ).astype(jnp.bfloat16)

    sent = windows(fields.reshape(rows, lanes, length), dom)
    parts = [sent[0]] + [swapped(sent[k], "dom", k) for k in range(1, dom)]
    pairs = evolve(cutoffs, diffusion, courant, (rate_high, rate_low), lane_surplus, parts, pieces, chain_orders)

    ends = []
    states = [(pairs[2 * c], pairs[2 * c + 1]) for c in range(len(chain_bits))]
    for step in range(len(halving)):
        arrived = [swapped(states[c][1], "grid", chain_bits[c][step]) for c in range(len(states))]
        last = step + 1 == len(halving)
        if last:
            ends = [(states[c][0][0], arrived[c][0]) for c in range(len(states))]
        else:
            for c in range(len(states)):
                added = states[c][0] + arrived[c]
                half = added.shape[0] // 2
                states[c] = (added[:half], added[half:])
    for bit in doubling:
        sums = [keep + arrived for keep, arrived in ends]
        ends = [(s, swapped(s, "grid", bit)) for s in sums]
    row_parts = rows_for(dom, 1.0 / grids, [a for end in ends for a in end])

    home = [row_parts[0]] + [swapped(row_parts[k], "dom", k) for k in range(1, dom)]
    arrays, groups = [], []
    gather_bits = [halving[::-1], halving[:1] + halving[:0:-1]]
    for c in range(2):
        ks = list(range(c * dom // 2, (c + 1) * dom // 2))
        held, slots = jnp.stack([home[k] for k in ks])[None], [0]
        for step, bit in enumerate(gather_bits[c]):
            arrived = swapped(held, "grid", bit)
            new_slots = [q | bit for q in slots]
            if step + 1 == len(gather_bits[c]):
                arrays += [held, arrived]
                groups += [(tuple(slots), tuple(ks)), (tuple(new_slots), tuple(ks))]
            else:
                held, slots = jnp.concatenate([held, arrived]), slots + new_slots
    out = restore(cutoffs, lane_restore, arrays, tuple(groups), dom, pieces, rows, lanes, length)
    return out.reshape(1, rows, second_len, third_len, length)


def solution(mesh):
    in_specs = (P("grid", "dom", None, None, None), P("grid", None), P("grid"), P(), P())
    out_specs = P("grid", "dom", None, None, None)
    return jax.shard_map(shards, mesh=mesh, in_specs=in_specs, out_specs=out_specs, check_vma=False)
```

```python
import functools

import jax
import jax.numpy as jnp
from jax import lax
from jax.experimental import pallas as pl
from jax.experimental.pallas import tpu as pltpu
from jax.sharding import PartitionSpec as P

STEPS = 2
HALO = 8
TILE = 8

VMEM = pl.BlockSpec(memory_space=pltpu.VMEM)
SMEM = pl.BlockSpec(memory_space=pltpu.SMEM)


def params(*arrays):
    held = sum(a.size * a.dtype.itemsize for a in arrays)
    return pltpu.CompilerParams(vmem_limit_bytes=min(2 * held + (4 << 20), 60 << 20))


def floats(*shape):
    return jax.ShapeDtypeStruct(shape, jnp.float32)


def swap_pairs(size, bit):
    return [(i, i ^ bit) for i in range(size)]


def swapped(x, axis, bit):
    return lax.ppermute(x, axis, swap_pairs(lax.axis_size(axis), bit))


def split_product(x, m_high, m_low=None, dims=(((1,), (0,)), ((), ()))):
    high = x.astype(jnp.bfloat16)
    low = (x - high.astype(jnp.float32)).astype(jnp.bfloat16)
    dot = functools.partial(lax.dot_general, dimension_numbers=dims, preferred_element_type=jnp.float32)
    total = dot(high, m_high) + dot(low, m_high)
    return total if m_low is None else total + dot(high, m_low)


def lane_places(second_len, third_len):
    shape = (second_len * third_len,) * 2
    row, col = (lax.broadcasted_iota(jnp.int32, shape, d) for d in (0, 1))
    return (row // third_len, col // third_len, second_len), (row % third_len, col % third_len, third_len)


def rate_matrix(second_len, third_len, diffusion, courant):
    (s_row, s_col, s_len), (t_row, t_col, t_len) = lane_places(second_len, third_len)

    def hop(row, col, length, by):
        return row == jnp.remainder(col + by, length)

    def where(cond, value):
        return jnp.where(cond, value, 0.0)

    same_s, same_t = s_row == s_col, t_row == t_col
    return (
        where(same_s & same_t, -2.0 * jnp.sum(diffusion))
        + where(hop(s_row, s_col, s_len, 1) & same_t, diffusion[1] - courant[1])
        + where(hop(s_row, s_col, s_len, -1) & same_t, diffusion[1] + courant[1])
        + where(hop(t_row, t_col, t_len, 1) & same_s, diffusion[2] - courant[2])
        + where(hop(t_row, t_col, t_len, -1) & same_s, diffusion[2] + courant[2])
    )


def surplus_entry(source, target, length):
    hop = jnp.where(target % 4 == 0, 0, jnp.where(target % 2 == 0, 2, 1))
    beside = (source == (target + hop) % length).astype(jnp.float32) + (source == (target - hop) % length).astype(
        jnp.float32
    )
    return (source == target).astype(jnp.float32) - jnp.where(hop > 0, 0.5, 0.0) * beside


def restore_entry(source, target, length):
    def at(by):
        return (source == (target + by) % length).astype(jnp.float32)

    lower, upper = (at(-1), at(1))
    inner = jnp.where(
        target % 4 == 1,
        0.75 * lower + 0.5 * upper + 0.25 * at(3),
        0.75 * upper + 0.5 * lower + 0.25 * at(-3),
    )
    beside = jnp.where(target % 4 == 0, 0.0, jnp.where(target % 4 == 2, 0.5 * (at(-2) + at(2)), inner))
    return at(0) + beside


def divides(place, cutoff):
    return (jnp.bitwise_and(place, jnp.left_shift(1, cutoff) - 1) == 0).astype(jnp.float32)


def windows_kernel(dom, u_ref, *refs):
    out_refs, ext = refs[:-1], refs[-1]
    rows, _, length = u_ref.shape
    block = length // dom
    width = block + 2 * HALO
    place = lax.axis_index("dom")
    for r in range(rows):
        turned = u_ref[r].T
        ext[pl.ds(HALO, length), :] = turned
        ext[pl.ds(0, HALO), :] = turned[length - HALO :]
        ext[pl.ds(HALO + length, HALO), :] = turned[:HALO]
        for k in range(dom):
            start = pl.multiple_of((place ^ k) * block, TILE)
            out_refs[k][r] = ext[pl.ds(start, width), :]


def windows(u, dom):
    rows, lanes, length = u.shape
    width = length // dom + 2 * HALO
    outs = [floats(rows, width, lanes)] * dom
    return pl.pallas_call(
        functools.partial(windows_kernel, dom),
        out_shape=outs,
        compiler_params=params(u, *outs),
        in_specs=[VMEM],
        out_specs=[VMEM] * dom,
        scratch_shapes=[pltpu.VMEM((length + 2 * HALO, lanes), jnp.float32)],
    )(u)


def evolve_kernel(plan, cut_ref, diff_ref, cour_ref, rate_high, rate_low, lane_surplus, *refs):
    dom, pieces, chain_orders, chunk = plan
    in_refs, refs = refs[:dom], refs[dom:]
    out_refs, (u, w1, w2) = refs[:-3], refs[-3:]
    rows = in_refs[0].shape[0]
    total, width, lanes = u.shape
    block = width - 2 * HALO
    place = lax.axis_index("dom")
    own = lax.axis_index("grid") & (pieces - 1)
    for k in range(dom):
        u[pl.ds((place ^ k) * rows, rows)] = in_refs[k][...]

    def stage(source, target, which, part):
        first = [part * (diff_ref[d] - cour_ref[d]) for d in (0, 3)]
        second = [part * (diff_ref[d] + cour_ref[d]) for d in (0, 3)]

        def body(c, carry):
            start = c * chunk
            here = [source[start + r] for r in range(chunk)]
            before = source[lax.rem(start + total - 1, total)]
            after = source[lax.rem(start + chunk, total)]
            flat = jnp.concatenate(here, axis=0)
            product = split_product(flat, rate_high[which], rate_low[which])
            for r in range(chunk):
                below = here[r - 1] if r else before
                above = here[r + 1] if r + 1 < chunk else after
                target[start + r] = (
                    u[start + r]
                    + product[r * width : (r + 1) * width]
                    + (first[0] * above + second[0] * below)
                    + (first[1] * pltpu.roll(here[r], width - 1, 0) + second[1] * pltpu.roll(here[r], 1, 0))
                )
            return carry

        lax.fori_loop(0, total // chunk, body, 0)

    for _ in range(STEPS):
        stage(u, w1, 0, 1.0 / 3.0)
        stage(w1, w2, 1, 0.5)
        stage(w2, u, 2, 1.0)

    cell = lax.broadcasted_iota(jnp.int32, (block, lanes), 0)
    kept = divides(cell, cut_ref[0, 3])
    odd, twice = cell % 2 == 1, cell % 4 == 2
    near = jnp.where(odd, -0.5, 0.0) * kept
    far = jnp.where(twice, -0.5, 0.0) * kept

    def lines(c, carry):
        start = c * chunk
        flat = jnp.concatenate([u[start + r] for r in range(chunk)], axis=0)
        product = split_product(flat, lane_surplus[...])
        for r in range(chunk):
            v = product[r * width : (r + 1) * width]

            def at(by):
                return pltpu.roll(v, (width - HALO - by) % width, 0)[:block]

            w1[start + r, pl.ds(0, block), :] = kept * at(0) + near * (at(1) + at(-1)) + far * (at(2) + at(-2))
        return carry

    lax.fori_loop(0, total // chunk, lines, 0)

    depth = block // pieces
    half = total // len(chain_orders)
    for chain, order in enumerate(chain_orders):
        keep_ref, send_ref = out_refs[2 * chain], out_refs[2 * chain + 1]
        for slot, q in enumerate(order):
            offset = pl.multiple_of((own ^ q) * depth, TILE)
            out, index = (keep_ref, slot) if slot < len(order) // 2 else (send_ref, slot - len(order) // 2)

            def row(i):
                return w1[i % total, pl.ds(offset, depth), :]

            for r in range(half):
                i = chain * half + r
                if i % 4 == 0:
                    out[index, r] = row(i)
                else:
                    hop = 2 if i % 2 == 0 else 1
                    scale = divides(jnp.int32(i), cut_ref[0, 0])
                    out[index, r] = scale * (row(i) - 0.5 * (row(i - hop) + row(i + hop)))


def evolve(cutoffs, diffusion, courant, rate_parts, lane_surplus, parts, pieces, chain_orders):
    dom = len(parts)
    rows, width, lanes = parts[0].shape
    total = rows * dom
    depth = (width - 2 * HALO) // pieces
    piece = (pieces // 2, total // len(chain_orders), depth, lanes)
    chunk = 4
    outs = [floats(*piece)] * (2 * len(chain_orders))
    return pl.pallas_call(
        functools.partial(evolve_kernel, (dom, pieces, chain_orders, chunk)),
        out_shape=outs,
        compiler_params=params(*parts, *outs, *[floats(total, width, lanes)] * 3),
        in_specs=[SMEM] * 3 + [VMEM] * (3 + dom),
        out_specs=[VMEM] * (2 * len(chain_orders)),
        scratch_shapes=[pltpu.VMEM((total, width, lanes), jnp.float32)] * 3,
    )(cutoffs, diffusion, courant, *rate_parts, lane_surplus, *parts)


def rows_kernel(dom, scale, *refs):
    chains = (len(refs) - dom) // 2
    out_refs = refs[2 * chains :]
    half = refs[0].shape[0]
    total = half * chains
    rows = total // dom
    place = lax.axis_index("dom")
    summed = [(refs[2 * c][...] + refs[2 * c + 1][...]) * scale for c in range(chains)]

    def body(all_rows):
        for c in range(chains):
            all_rows[pl.ds(c * half, half)] = summed[c]
        all_rows[pl.ds(total, 1)] = summed[0][:1]
        for k in range(dom):
            out_refs[k][...] = all_rows[pl.ds((place ^ k) * rows, rows + 1)]

    pl.run_scoped(body, pltpu.VMEM((total + 1, *refs[0].shape[1:]), jnp.float32))


def rows_for(dom, scale, ends):
    half, depth, lanes = ends[0].shape
    rows = half * len(ends) // 2 // dom
    outs = [floats(rows + 1, depth, lanes)] * dom
    return pl.pallas_call(
        functools.partial(rows_kernel, dom, scale),
        out_shape=outs,
        compiler_params=params(*ends, *outs),
        in_specs=[VMEM] * len(ends),
        out_specs=[VMEM] * dom,
    )(*ends)


def restore_kernel(plan, cut_ref, lane_restore, *refs):
    dom, pieces, groups = plan
    in_refs, out_ref, summed = refs[:-2], refs[-2], refs[-1]
    rows, lanes, length = out_ref.shape
    place = lax.axis_index("dom")
    own = lax.axis_index("grid") & (pieces - 1)
    depth = length // (dom * pieces)
    for ref, (slots, ks) in zip(in_refs, groups):
        for s, q in enumerate(slots):
            for m, k in enumerate(ks):
                at = pl.multiple_of(((place ^ k) * pieces + (own ^ q)) * depth, TILE)
                summed[:, pl.ds(at, depth), :] = ref[s, m]

    cell = lax.broadcasted_iota(jnp.int32, (length, lanes), 0)
    kept = divides(cell, cut_ref[0, 3])
    odd, twice = cell % 2 == 1, cell % 4 == 2
    far = jnp.where(twice, 0.5, 0.0)
    near = jnp.where(odd, 0.5, 0.0)

    def along_cells(v):
        v = kept * v
        v = v + far * (pltpu.roll(v, length - 2, 0) + pltpu.roll(v, 2, 0))
        v = v + near * (pltpu.roll(v, length - 1, 0) + pltpu.roll(v, 1, 0))
        high = v.astype(jnp.bfloat16)
        low = (v - high.astype(jnp.float32)).astype(jnp.bfloat16)
        dims = (((1,), (1,)), ((), ()))
        dot = functools.partial(lax.dot_general, dimension_numbers=dims, preferred_element_type=jnp.float32)
        return dot(lane_restore[...], high) + dot(lane_restore[...], low)

    one = divides(jnp.int32(1), cut_ref[0, 0])
    two = divides(jnp.int32(2), cut_ref[0, 0])
    for r in range(0, rows, 4):
        first, last = summed[r], summed[r + 4]
        middle = two * summed[r + 2] + 0.5 * (first + last)
        out_ref[r] = along_cells(first)
        out_ref[r + 1] = along_cells(one * summed[r + 1] + 0.5 * (first + middle))
        out_ref[r + 2] = along_cells(middle)
        out_ref[r + 3] = along_cells(one * summed[r + 3] + 0.5 * (middle + last))


def restore(cutoffs, lane_restore, arrays, groups, dom, pieces, rows, lanes, length):
    out = floats(rows, lanes, length)
    return pl.pallas_call(
        functools.partial(restore_kernel, (dom, pieces, groups)),
        out_shape=out,
        compiler_params=params(*arrays, out, floats(rows + 1, length, lanes)),
        in_specs=[SMEM, VMEM] + [VMEM] * len(arrays),
        out_specs=VMEM,
        scratch_shapes=[pltpu.VMEM((rows + 1, length, lanes), jnp.float32)],
    )(cutoffs, lane_restore, *arrays)


def slot_order(bits):
    order = [0]
    for bit in reversed(bits):
        order = order + [q | bit for q in order]
    return order


def shards(fields, cutoffs, weights, diffusion, courant):
    rows, second_len, third_len, length = fields.shape[1:]
    lanes = second_len * third_len
    dom, grids = lax.axis_size("dom"), lax.axis_size("grid")
    block = length // dom
    pieces = min(grids, block // TILE)
    bits = [1 << i for i in range(grids.bit_length() - 1)]
    halving = [b for b in bits if b < pieces]
    doubling = [b for b in bits if b >= pieces]
    chain_bits = [halving, halving[1:] + halving[:1]]
    chain_orders = tuple(tuple(slot_order(b)) for b in chain_bits)

    base = rate_matrix(second_len, third_len, diffusion, courant)
    rate = jnp.stack([base / 3.0, base * 0.5, base])
    rounded = lax.reduce_precision(rate, exponent_bits=8, mantissa_bits=7)
    rate_high, rate_low = rounded.astype(jnp.bfloat16), (rate - rounded).astype(jnp.bfloat16)
    (s_row, s_col, s_len), (t_row, t_col, t_len) = lane_places(second_len, third_len)
    cut = cutoffs[0]
    lane_surplus = (
        surplus_entry(s_row, s_col, s_len)
        * surplus_entry(t_row, t_col, t_len)
        * (divides(s_col, cut[1]) * divides(t_col, cut[2]))
        * weights[0].astype(jnp.float32)
    ).astype(jnp.bfloat16)
    lane_restore = (
        restore_entry(s_col, s_row, s_len)
        * restore_entry(t_col, t_row, t_len)
        * (divides(s_col, cut[1]) * divides(t_col, cut[2]))
    ).astype(jnp.bfloat16)

    sent = windows(fields.reshape(rows, lanes, length), dom)
    parts = [sent[0]] + [swapped(sent[k], "dom", k) for k in range(1, dom)]
    pairs = evolve(cutoffs, diffusion, courant, (rate_high, rate_low), lane_surplus, parts, pieces, chain_orders)

    ends = []
    states = [(pairs[2 * c], pairs[2 * c + 1]) for c in range(len(chain_bits))]
    for step in range(len(halving)):
        arrived = [swapped(states[c][1], "grid", chain_bits[c][step]) for c in range(len(states))]
        last = step + 1 == len(halving)
        if last:
            ends = [(states[c][0][0], arrived[c][0]) for c in range(len(states))]
        else:
            for c in range(len(states)):
                added = states[c][0] + arrived[c]
                half = added.shape[0] // 2
                states[c] = (added[:half], added[half:])
    for bit in doubling:
        sums = [keep + arrived for keep, arrived in ends]
        ends = [(s, swapped(s, "grid", bit)) for s in sums]
    row_parts = rows_for(dom, 1.0 / grids, [a for end in ends for a in end])

    home = [row_parts[0]] + [swapped(row_parts[k], "dom", k) for k in range(1, dom)]
    arrays, groups = [], []
    gather_bits = [halving[::-1], halving[:1] + halving[:0:-1]]
    for c in range(2):
        ks = list(range(c * dom // 2, (c + 1) * dom // 2))
        held, slots = jnp.stack([home[k] for k in ks])[None], [0]
        for step, bit in enumerate(gather_bits[c]):
            arrived = swapped(held, "grid", bit)
            new_slots = [q | bit for q in slots]
            if step + 1 == len(gather_bits[c]):
                arrays += [held, arrived]
                groups += [(tuple(slots), tuple(ks)), (tuple(new_slots), tuple(ks))]
            else:
                held, slots = jnp.concatenate([held, arrived]), slots + new_slots
    out = restore(cutoffs, lane_restore, arrays, tuple(groups), dom, pieces, rows, lanes, length)
    return out.reshape(1, rows, second_len, third_len, length)


def solution(mesh):
    in_specs = (P("grid", "dom", None, None, None), P("grid", None), P("grid"), P(), P())
    out_specs = P("grid", "dom", None, None, None)
    return jax.shard_map(shards, mesh=mesh, in_specs=in_specs, out_specs=out_specs, check_vma=False)
```

```python
import functools

import jax
import jax.numpy as jnp
from jax import lax
from jax.experimental import pallas as pl
from jax.experimental.pallas import tpu as pltpu
from jax.sharding import PartitionSpec as P

STEPS = 2
HALO = 8
TILE = 8
LANES = 128
CHAINS = 2

VMEM = pl.BlockSpec(memory_space=pltpu.VMEM)
SMEM = pl.BlockSpec(memory_space=pltpu.SMEM)


def params(*arrays):
    held = sum(a.size * a.dtype.itemsize for a in arrays)
    return pltpu.CompilerParams(vmem_limit_bytes=min(2 * held + (4 << 20), 60 << 20))


def floats(*shape):
    return jax.ShapeDtypeStruct(shape, jnp.float32)


def swap_pairs(size, bit):
    return [(i, i ^ bit) for i in range(size)]


def swapped(x, axis, bit):
    return lax.ppermute(x, axis, swap_pairs(lax.axis_size(axis), bit))


def halves(x):
    high = x.astype(jnp.bfloat16)
    return high, (x - high.astype(jnp.float32)).astype(jnp.bfloat16)


def split_product(x, m_high, m_low=None):
    high, low = halves(x)
    dot = functools.partial(jnp.dot, preferred_element_type=jnp.float32)
    total = dot(high, m_high) + dot(low, m_high)
    return total if m_low is None else total + dot(high, m_low)


def divides(place, cutoff):
    return (jnp.bitwise_and(place, jnp.left_shift(1, cutoff) - 1) == 0).astype(jnp.float32)


def grid_piece(bits):
    place = lax.axis_index("grid")
    return sum(jnp.bitwise_and(lax.div(place, bit), 1) * (1 << i) for i, bit in enumerate(bits))


def surplus_entry(source, target, length):
    low = jnp.bitwise_and(target, 3)
    hop = jnp.where(low == 0, 0, jnp.where(low == 2, 2, 1))
    gap = jnp.bitwise_and(source - target, length - 1)
    beside = (gap == hop).astype(jnp.float32) + (gap == jnp.bitwise_and(-hop, length - 1)).astype(jnp.float32)
    return (gap == 0).astype(jnp.float32) - jnp.where(hop > 0, 0.5, 0.0) * beside


def restore_entry(source, target, length):
    low = jnp.bitwise_and(target, 3)
    gap = jnp.bitwise_and(source - target, length - 1)

    def at(by):
        return (gap == by % length).astype(jnp.float32)

    one = 0.75 * at(-1) + 0.5 * at(1) + 0.25 * at(3)
    three = 0.75 * at(1) + 0.5 * at(-1) + 0.25 * at(-3)
    two = 0.5 * (at(-2) + at(2))
    beside = jnp.where(low == 0, 0.0, jnp.where(low == 2, two, jnp.where(low == 1, one, three)))
    return at(0) + beside


def tables_kernel(lens, cut_ref, weight_ref, diff_ref, cour_ref, rate_high, rate_low, surplus_ref, restore_ref):
    second_len, third_len = lens
    shape = surplus_ref.shape
    row, col = (lax.broadcasted_iota(jnp.int32, shape, d) for d in (0, 1))
    shift = third_len.bit_length() - 1
    s_row, s_col = jnp.right_shift(row, shift), jnp.right_shift(col, shift)
    t_row, t_col = jnp.bitwise_and(row, third_len - 1), jnp.bitwise_and(col, third_len - 1)
    s_gap = jnp.bitwise_and(s_row - s_col, second_len - 1)
    t_gap = jnp.bitwise_and(t_row - t_col, third_len - 1)

    def where(cond, value):
        return jnp.where(cond, value, 0.0)

    spread = diff_ref[0] + diff_ref[1] + diff_ref[2] + diff_ref[3]
    rate = where((s_gap == 0) & (t_gap == 0), -2.0 * spread)
    rate += where((s_gap == 1) & (t_gap == 0), diff_ref[1] - cour_ref[1])
    rate += where((s_gap == second_len - 1) & (t_gap == 0), diff_ref[1] + cour_ref[1])
    rate += where((t_gap == 1) & (s_gap == 0), diff_ref[2] - cour_ref[2])
    rate += where((t_gap == third_len - 1) & (s_gap == 0), diff_ref[2] + cour_ref[2])
    for which, part in enumerate((1.0 / 3.0, 0.5, 1.0)):
        rate_high[which], rate_low[which] = halves(rate * part)

    kept = divides(s_col, cut_ref[0, 1]) * divides(t_col, cut_ref[0, 2])
    entry = surplus_entry(s_row, s_col, second_len) * surplus_entry(t_row, t_col, third_len)
    surplus_ref[...] = (kept * weight_ref[0].astype(jnp.float32) * entry).astype(jnp.bfloat16)
    entry = restore_entry(s_col, s_row, second_len) * restore_entry(t_col, t_row, third_len)
    restore_ref[...] = (kept * entry).astype(jnp.bfloat16)


def tables(cutoffs, weights, diffusion, courant, second_len, third_len):
    lanes = second_len * third_len
    one = jax.ShapeDtypeStruct((lanes, lanes), jnp.bfloat16)
    three = jax.ShapeDtypeStruct((3, lanes, lanes), jnp.bfloat16)
    outs = [three, three, one, one]
    return pl.pallas_call(
        functools.partial(tables_kernel, (second_len, third_len)),
        out_shape=outs,
        in_specs=[SMEM] * 4,
        out_specs=[VMEM] * 4,
        compiler_params=params(*outs),
    )(cutoffs, weights, diffusion, courant)


def windows_kernel(dom, u_ref, *refs):
    out_refs, ext = refs[:-1], refs[-1]
    rows, _, length = u_ref.shape
    block = length // dom
    place = lax.axis_index("dom")
    for r in range(rows):
        turned = u_ref[r].T
        ext[r, pl.ds(HALO, length), :] = turned
        ext[r, pl.ds(0, HALO), :] = turned[length - HALO :]
        ext[r, pl.ds(HALO + length, HALO), :] = turned[:HALO]
    for k in range(dom):
        start = pl.multiple_of((place ^ k) * block, TILE)
        for c in range(CHAINS):
            out = out_refs[c * dom + k]
            out[...] = ext[:, pl.ds(start, out.shape[1]), :]
            start += out.shape[1]


def windows(u, dom):
    rows, lanes, length = u.shape
    sub = length // dom // CHAINS
    outs = [floats(rows, sub + 2 * HALO if c == 0 else sub, lanes) for c in range(CHAINS) for _ in range(dom)]
    ext = (rows, length + 2 * HALO, lanes)
    sent = pl.pallas_call(
        functools.partial(windows_kernel, dom),
        out_shape=outs,
        in_specs=[VMEM],
        out_specs=[VMEM] * len(outs),
        scratch_shapes=[pltpu.VMEM(ext, jnp.float32)],
        compiler_params=params(u, floats(*ext), *outs),
    )(u)
    return [sent[c * dom : (c + 1) * dom] for c in range(CHAINS)]


def evolve_kernel(plan, cut_ref, diff_ref, cour_ref, rate_high, rate_low, lane_surplus, *refs):
    dom, bits, order, chunk, arrays = plan
    in_refs, refs = refs[: dom * arrays], refs[dom * arrays :]
    out_refs, (u, w1, w2) = refs[:-3], refs[-3:]
    rows, lanes = in_refs[0].shape[0], in_refs[0].shape[2]
    tiles, total, width, _ = u.shape
    width -= 2 * TILE
    sub = width - 2 * HALO
    place = lax.axis_index("dom")
    body_rows = pl.ds(TILE, width)
    for k in range(dom):
        at, need = TILE + width, width
        for a in reversed(range(arrays)):
            part = in_refs[a * dom + k]
            take = min(need, part.shape[1])
            at, need = at - take, need - take
            for h in range(tiles):
                u[h, pl.ds((place ^ k) * rows, rows), pl.ds(at, take), :] = part[
                    :, pl.ds(part.shape[1] - take, take), pl.ds(h * LANES, LANES)
                ]
    spare = jnp.zeros((tiles, total, TILE, LANES), jnp.float32)
    for ref in (u, w1, w2):
        ref[:, :, pl.ds(0, TILE), :] = spare
        ref[:, :, pl.ds(TILE + width, TILE), :] = spare

    def flat_rows(source, start):
        return jnp.concatenate(
            [
                jnp.concatenate([source[h, start + r, body_rows, :] for h in range(tiles)], axis=1)
                for r in range(chunk)
            ],
            axis=0,
        )

    def cut_rows(product, r, h):
        return product[r * width : (r + 1) * width, h * LANES : (h + 1) * LANES]

    def loop(body):
        if total == chunk:
            body(0)
        else:
            lax.fori_loop(0, total // chunk, lambda c, carry: (body(c * chunk), carry)[1], 0)

    def stage(source, target, which, part):
        first = [part * (diff_ref[d] - cour_ref[d]) for d in (0, 3)]
        second = [part * (diff_ref[d] + cour_ref[d]) for d in (0, 3)]

        def body(start):
            product = split_product(flat_rows(source, start), rate_high[which], rate_low[which])
            for r in range(chunk):
                i = start + r
                above = lax.rem(i + 1, total) if r + 1 == chunk else i + 1
                below = lax.rem(i + total - 1, total) if r == 0 else i - 1
                for h in range(tiles):
                    target[h, i, body_rows, :] = (
                        u[h, i, body_rows, :]
                        + cut_rows(product, r, h)
                        + (first[0] * source[h, above, body_rows, :] + second[0] * source[h, below, body_rows, :])
                        + (
                            first[1] * source[h, i, pl.ds(TILE + 1, width), :]
                            + second[1] * source[h, i, pl.ds(TILE - 1, width), :]
                        )
                    )

        loop(body)

    for _ in range(STEPS):
        stage(u, w1, 0, 1.0 / 3.0)
        stage(w1, w2, 1, 0.5)
        stage(w2, u, 2, 1.0)

    cell = lax.broadcasted_iota(jnp.int32, (sub, LANES), 0)
    low = jnp.bitwise_and(cell, 3)
    kept = divides(cell, cut_ref[0, 3])
    near = jnp.where(jnp.bitwise_and(low, 1) == 1, -0.5, 0.0) * kept
    far = jnp.where(low == 2, -0.5, 0.0) * kept

    def lines(start):
        product = split_product(flat_rows(u, start), lane_surplus[...])
        for r in range(chunk):
            for h in range(tiles):
                w1[h, start + r, body_rows, :] = cut_rows(product, r, h)
                at = [w1[h, start + r, pl.ds(TILE + HALO + by, sub), :] for by in (-2, -1, 0, 1, 2)]
                w2[h, start + r, pl.ds(TILE, sub), :] = (
                    kept * at[2] + near * (at[1] + at[3]) + far * (at[0] + at[4])
                )

    loop(lines)

    pieces = len(order)
    depth = sub // pieces
    own = grid_piece(bits)
    scales = {2: divides(jnp.int32(2), cut_ref[0, 0]), 1: divides(jnp.int32(1), cut_ref[0, 0])}
    for slot, q in enumerate(order):
        offset = pl.multiple_of(TILE + (own ^ q) * depth, TILE)
        out, index = out_refs[slot // out_refs[0].shape[0]], slot % out_refs[0].shape[0]
        for h in range(tiles):
            line = [w2[h, i, pl.ds(offset, depth), :] for i in range(total)]
            for i in range(total):
                value = line[i]
                if i % 4:
                    hop = 2 if i % 2 == 0 else 1
                    value = scales[hop] * (value - 0.5 * (line[i - hop] + line[(i + hop) % total]))
                out[index, i, :, pl.ds(h * LANES, LANES)] = value


def evolve(cutoffs, diffusion, courant, mats, parts, bits, order):
    dom, arrays = len(parts[0]), len(parts)
    rows, lanes = parts[0][0].shape[0], parts[0][0].shape[2]
    sub = min(p[0].shape[1] for p in parts)
    if arrays == 1:
        sub -= 2 * HALO
    total = rows * dom
    width = sub + 2 * HALO
    pieces = len(order)
    kept = max(pieces // 2, 1)
    outs = [floats(kept, total, sub // pieces, lanes)] * min(pieces, 2)
    state = (lanes // LANES, total, width + 2 * TILE, LANES)
    chunk = min(8, total)
    flat = [p for part in parts for p in part]
    return pl.pallas_call(
        functools.partial(evolve_kernel, (dom, bits, order, chunk, arrays)),
        out_shape=outs,
        in_specs=[SMEM] * 3 + [VMEM] * (3 + len(flat)),
        out_specs=[VMEM] * len(outs),
        scratch_shapes=[pltpu.VMEM(state, jnp.float32)] * 3,
        compiler_params=params(*flat, *outs, *[floats(*state)] * 3),
    )(cutoffs, diffusion, courant, *mats, *flat)


def rows_kernel(dom, scale, *refs):
    in_refs, out_refs = refs[:-dom], refs[-dom:]
    total = in_refs[0].shape[0]
    rows = total // dom
    place = lax.axis_index("dom")

    def row(i):
        value = in_refs[0][pl.ds(i, 1)]
        for ref in in_refs[1:]:
            value += ref[pl.ds(i, 1)]
        return value * scale

    for k in range(dom):
        first = (place ^ k) * rows
        for r in range(rows + 1):
            i = first + r if r < rows else lax.rem(first + rows, total)
            out_refs[k][pl.ds(r, 1)] = row(i)


def rows_for(dom, scale, addends):
    total, depth, lanes = addends[0].shape
    outs = [floats(total // dom + 1, depth, lanes)] * dom
    return pl.pallas_call(
        functools.partial(rows_kernel, dom, scale),
        out_shape=outs,
        in_specs=[VMEM] * len(addends),
        out_specs=[VMEM] * dom,
        compiler_params=params(*addends, *outs),
    )(*addends)


def restore_kernel(plan, cut_ref, lane_restore, *refs):
    dom, groups = plan
    in_refs, out_ref, summed = refs[:-2], refs[-2], refs[-1]
    rows, lanes, length = out_ref.shape
    place = lax.axis_index("dom")
    block = length // dom
    for ref, (chain, bits, slots) in zip(in_refs, groups):
        depth = block // CHAINS >> len(bits)
        own = grid_piece(bits)
        for s, q in enumerate(slots):
            for k in range(dom):
                at = (place ^ k) * block + chain * (block // CHAINS) + (own ^ q) * depth
                summed[:, pl.ds(pl.multiple_of(at, TILE), depth), :] = ref[s, k]

    cell = lax.broadcasted_iota(jnp.int32, (length, lanes), 0)
    low = jnp.bitwise_and(cell, 3)
    kept = divides(cell, cut_ref[0, 3])
    far = jnp.where(low == 2, 0.5, 0.0)
    near = jnp.where(jnp.bitwise_and(low, 1) == 1, 0.5, 0.0)

    def along_cells(v):
        v = kept * v
        v = v + far * (pltpu.roll(v, length - 2, 0) + pltpu.roll(v, 2, 0))
        v = v + near * (pltpu.roll(v, length - 1, 0) + pltpu.roll(v, 1, 0))
        high, low_part = halves(v)
        dims = (((1,), (1,)), ((), ()))
        dot = functools.partial(lax.dot_general, dimension_numbers=dims, preferred_element_type=jnp.float32)
        return dot(lane_restore[...], high) + dot(lane_restore[...], low_part)

    one = divides(jnp.int32(1), cut_ref[0, 0])
    two = divides(jnp.int32(2), cut_ref[0, 0])
    for r in range(0, rows, 4):
        first, last = summed[r], summed[r + 4]
        middle = two * summed[r + 2] + 0.5 * (first + last)
        out_ref[r] = along_cells(first)
        out_ref[r + 1] = along_cells(one * summed[r + 1] + 0.5 * (first + middle))
        out_ref[r + 2] = along_cells(middle)
        out_ref[r + 3] = along_cells(one * summed[r + 3] + 0.5 * (middle + last))


def restore(cutoffs, lane_restore, arrays, groups, dom, rows, lanes, length):
    out = floats(rows, lanes, length)
    return pl.pallas_call(
        functools.partial(restore_kernel, (dom, groups)),
        out_shape=out,
        in_specs=[SMEM, VMEM] + [VMEM] * len(arrays),
        out_specs=VMEM,
        scratch_shapes=[pltpu.VMEM((rows + 1, length, lanes), jnp.float32)],
        compiler_params=params(*arrays, out, floats(rows + 1, length, lanes)),
    )(cutoffs, lane_restore, *arrays)


def slot_order(count):
    order = [0]
    for i in reversed(range(count)):
        order = order + [q | 1 << i for q in order]
    return tuple(order)


def grid_sum(first, halving, doubling):
    state = list(first)
    for bit in halving[:-1]:
        added = state[0] + swapped(state[1], "grid", bit)
        half = added.shape[0] // 2
        state = [added[:half], added[half:]]
    addends = [state[0][0]]
    if halving:
        addends.append(swapped(state[1], "grid", halving[-1])[0])
    for bit in doubling:
        own = sum(addends[1:], addends[0])
        addends = [own, swapped(own, "grid", bit)]
    return addends


def shards(fields, cutoffs, weights, diffusion, courant):
    rows, second_len, third_len, length = fields.shape[1:]
    lanes = second_len * third_len
    dom, grids = lax.axis_size("dom"), lax.axis_size("grid")
    sub = length // dom // CHAINS
    count = min(grids.bit_length(), (sub // TILE).bit_length()) - 1
    grid_bits = [1 << i for i in range(grids.bit_length() - 1)]

    sent = windows(fields.reshape(rows, lanes, length), dom)
    mats = tables(cutoffs, weights, diffusion, courant, second_len, third_len)
    parts = [[s[0]] + [swapped(s[k], "dom", k) for k in range(1, dom)] for s in sent]

    arrays, groups = [], []
    for c in range(CHAINS):
        bits = grid_bits[c:] + grid_bits[:c]
        halving, doubling = tuple(bits[:count]), tuple(bits[count:])
        order = slot_order(count)
        first = evolve(cutoffs, diffusion, courant, mats[:3], parts[: c + 1][-2:], halving, order)
        addends = grid_sum(first, halving, doubling)
        needed = rows_for(dom, 1.0 / grids, addends)
        home = [needed[0]] + [swapped(needed[k], "dom", k) for k in range(1, dom)]
        held, slots = jnp.stack(home)[None], [0]
        for i in reversed(range(count)):
            arrived = swapped(held, "grid", halving[i])
            new_slots = [q | 1 << i for q in slots]
            if i == 0:
                arrays += [held, arrived]
                groups += [(c, halving, tuple(slots)), (c, halving, tuple(new_slots))]
            else:
                held, slots = jnp.concatenate([held, arrived]), slots + new_slots
        if not count:
            arrays.append(held)
            groups.append((c, halving, (0,)))
    out = restore(cutoffs, mats[3], arrays, tuple(groups), dom, rows, lanes, length)
    return out.reshape(1, rows, second_len, third_len, length)


def solution(mesh):
    in_specs = (P("grid", "dom", None, None, None), P("grid", None), P("grid"), P(), P())
    out_specs = P("grid", "dom", None, None, None)
    return jax.shard_map(shards, mesh=mesh, in_specs=in_specs, out_specs=out_specs, check_vma=False)
```

```python
import functools

import jax
import jax.numpy as jnp
from jax import lax
from jax.experimental import pallas as pl
from jax.experimental.pallas import tpu as pltpu
from jax.sharding import PartitionSpec as P

STEPS = 2
HALO = 8
TILE = 8
LANES = 128
CHAINS = 2

VMEM = pl.BlockSpec(memory_space=pltpu.VMEM)
SMEM = pl.BlockSpec(memory_space=pltpu.SMEM)


def params(*arrays):
    held = sum(a.size * a.dtype.itemsize for a in arrays)
    return pltpu.CompilerParams(vmem_limit_bytes=min(2 * held + (4 << 20), 60 << 20))


def floats(*shape):
    return jax.ShapeDtypeStruct(shape, jnp.float32)


def swapped(x, axis, bit):
    size = lax.axis_size(axis)
    return lax.ppermute(x, axis, [(i, i ^ bit) for i in range(size)])


def turned(i, core, count):
    return (i + core) % count


def swapped_in_turn(x, i, count):
    grids, dom = lax.axis_size("grid"), lax.axis_size("dom")
    pairs = []
    for g in range(grids):
        for d in range(dom):
            pairs.append((g * dom + d, (g ^ 1 << turned(i, d & 1, count)) * dom + d))
    return lax.ppermute(x, ("grid", "dom"), pairs)


def halves(x):
    high = x.astype(jnp.bfloat16)
    return high, (x - high.astype(jnp.float32)).astype(jnp.bfloat16)


def split_product(x, m_high, m_low=None):
    high, low = halves(x)
    dot = functools.partial(jnp.dot, preferred_element_type=jnp.float32)
    total = dot(high, m_high) + dot(low, m_high)
    return total if m_low is None else total + dot(high, m_low)


def divides(place, cutoff):
    return (jnp.bitwise_and(place, jnp.left_shift(1, cutoff) - 1) == 0).astype(jnp.float32)


def piece_at(slot, count):
    place, core = lax.axis_index("grid"), jnp.bitwise_and(lax.axis_index("dom"), 1)
    piece = jnp.bitwise_and(place, (1 << count) - 1)
    for i in range(count):
        if slot >> i & 1:
            piece = piece ^ jnp.left_shift(1, lax.rem(i + core, count))
    return piece


def surplus_entry(source, target, length):
    low = jnp.bitwise_and(target, 3)
    hop = jnp.where(low == 0, 0, jnp.where(low == 2, 2, 1))
    gap = jnp.bitwise_and(source - target, length - 1)
    beside = (gap == hop).astype(jnp.float32) + (gap == jnp.bitwise_and(-hop, length - 1)).astype(jnp.float32)
    return (gap == 0).astype(jnp.float32) - jnp.where(hop > 0, 0.5, 0.0) * beside


def restore_entry(source, target, length):
    low = jnp.bitwise_and(target, 3)
    gap = jnp.bitwise_and(source - target, length - 1)

    def at(by):
        return (gap == by % length).astype(jnp.float32)

    one = 0.75 * at(-1) + 0.5 * at(1) + 0.25 * at(3)
    three = 0.75 * at(1) + 0.5 * at(-1) + 0.25 * at(-3)
    two = 0.5 * (at(-2) + at(2))
    beside = jnp.where(low == 0, 0.0, jnp.where(low == 2, two, jnp.where(low == 1, one, three)))
    return at(0) + beside


def tables_kernel(lens, cut_ref, weight_ref, diff_ref, cour_ref, rate_high, rate_low, surplus_ref, restore_ref):
    second_len, third_len = lens
    shape = surplus_ref.shape
    row, col = (lax.broadcasted_iota(jnp.int32, shape, d) for d in (0, 1))
    shift = third_len.bit_length() - 1
    s_row, s_col = jnp.right_shift(row, shift), jnp.right_shift(col, shift)
    t_row, t_col = jnp.bitwise_and(row, third_len - 1), jnp.bitwise_and(col, third_len - 1)
    s_gap = jnp.bitwise_and(s_row - s_col, second_len - 1)
    t_gap = jnp.bitwise_and(t_row - t_col, third_len - 1)

    def where(cond, value):
        return jnp.where(cond, value, 0.0)

    spread = diff_ref[0] + diff_ref[1] + diff_ref[2] + diff_ref[3]
    rate = where((s_gap == 0) & (t_gap == 0), -2.0 * spread)
    rate += where((s_gap == 1) & (t_gap == 0), diff_ref[1] - cour_ref[1])
    rate += where((s_gap == second_len - 1) & (t_gap == 0), diff_ref[1] + cour_ref[1])
    rate += where((t_gap == 1) & (s_gap == 0), diff_ref[2] - cour_ref[2])
    rate += where((t_gap == third_len - 1) & (s_gap == 0), diff_ref[2] + cour_ref[2])
    for which, part in enumerate((1.0 / 3.0, 0.5, 1.0)):
        rate_high[which], rate_low[which] = halves(rate * part)

    kept = divides(s_col, cut_ref[0, 1]) * divides(t_col, cut_ref[0, 2])
    entry = surplus_entry(s_row, s_col, second_len) * surplus_entry(t_row, t_col, third_len)
    surplus_ref[...] = (kept * weight_ref[0].astype(jnp.float32) * entry).astype(jnp.bfloat16)
    entry = restore_entry(s_col, s_row, second_len) * restore_entry(t_col, t_row, third_len)
    restore_ref[...] = (kept * entry).astype(jnp.bfloat16)


def tables(cutoffs, weights, diffusion, courant, second_len, third_len):
    lanes = second_len * third_len
    one = jax.ShapeDtypeStruct((lanes, lanes), jnp.bfloat16)
    three = jax.ShapeDtypeStruct((3, lanes, lanes), jnp.bfloat16)
    outs = [three, three, one, one]
    return pl.pallas_call(
        functools.partial(tables_kernel, (second_len, third_len)),
        out_shape=outs,
        in_specs=[SMEM] * 4,
        out_specs=[VMEM] * 4,
        compiler_params=params(*outs),
    )(cutoffs, weights, diffusion, courant)


def windows_kernel(dom, u_ref, *refs):
    out_refs, ext = refs[:-1], refs[-1]
    rows, _, length = u_ref.shape
    block = length // dom
    place = lax.axis_index("dom")
    for r in range(rows):
        turned = u_ref[r].T
        ext[r, pl.ds(HALO, length), :] = turned
        ext[r, pl.ds(0, HALO), :] = turned[length - HALO :]
        ext[r, pl.ds(HALO + length, HALO), :] = turned[:HALO]
    for k in range(dom):
        start = pl.multiple_of((place ^ k) * block, TILE)
        for c in range(CHAINS):
            out = out_refs[c * dom + k]
            out[...] = ext[:, pl.ds(start, out.shape[1]), :]
            start += out.shape[1]


def windows(u, dom):
    rows, lanes, length = u.shape
    sub = length // dom // CHAINS
    outs = [floats(rows, sub + 2 * HALO if c == 0 else sub, lanes) for c in range(CHAINS) for _ in range(dom)]
    ext = (rows, length + 2 * HALO, lanes)
    sent = pl.pallas_call(
        functools.partial(windows_kernel, dom),
        out_shape=outs,
        in_specs=[VMEM],
        out_specs=[VMEM] * len(outs),
        scratch_shapes=[pltpu.VMEM(ext, jnp.float32)],
        compiler_params=params(u, floats(*ext), *outs),
    )(u)
    return [sent[c * dom : (c + 1) * dom] for c in range(CHAINS)]


def evolve_kernel(plan, cut_ref, diff_ref, cour_ref, rate_high, rate_low, lane_surplus, *refs):
    dom, order, chunk, arrays = plan
    in_refs, refs = refs[: dom * arrays], refs[dom * arrays :]
    out_refs, (u, w1, w2) = refs[:-3], refs[-3:]
    rows, lanes = in_refs[0].shape[0], in_refs[0].shape[2]
    tiles, total, width, _ = u.shape
    width -= 2 * TILE
    sub = width - 2 * HALO
    place = lax.axis_index("dom")
    body_rows = pl.ds(TILE, width)
    for k in range(dom):
        at, need = TILE + width, width
        for a in reversed(range(arrays)):
            part = in_refs[a * dom + k]
            take = min(need, part.shape[1])
            at, need = at - take, need - take
            for h in range(tiles):
                u[h, pl.ds((place ^ k) * rows, rows), pl.ds(at, take), :] = part[
                    :, pl.ds(part.shape[1] - take, take), pl.ds(h * LANES, LANES)
                ]
    spare = jnp.zeros((tiles, total, TILE, LANES), jnp.float32)
    for ref in (u, w1, w2):
        ref[:, :, pl.ds(0, TILE), :] = spare
        ref[:, :, pl.ds(TILE + width, TILE), :] = spare

    def flat_rows(source, start):
        return jnp.concatenate(
            [
                jnp.concatenate([source[h, start + r, body_rows, :] for h in range(tiles)], axis=1)
                for r in range(chunk)
            ],
            axis=0,
        )

    def cut_rows(product, r, h):
        return product[r * width : (r + 1) * width, h * LANES : (h + 1) * LANES]

    def loop(body):
        if total == chunk:
            body(0)
        else:
            lax.fori_loop(0, total // chunk, lambda c, carry: (body(c * chunk), carry)[1], 0)

    def stage(source, target, which, part):
        first = [part * (diff_ref[d] - cour_ref[d]) for d in (0, 3)]
        second = [part * (diff_ref[d] + cour_ref[d]) for d in (0, 3)]

        def body(start):
            product = split_product(flat_rows(source, start), rate_high[which], rate_low[which])
            for r in range(chunk):
                i = start + r
                above = lax.rem(i + 1, total) if r + 1 == chunk else i + 1
                below = lax.rem(i + total - 1, total) if r == 0 else i - 1
                for h in range(tiles):
                    target[h, i, body_rows, :] = (
                        u[h, i, body_rows, :]
                        + cut_rows(product, r, h)
                        + (first[0] * source[h, above, body_rows, :] + second[0] * source[h, below, body_rows, :])
                        + (
                            first[1] * source[h, i, pl.ds(TILE + 1, width), :]
                            + second[1] * source[h, i, pl.ds(TILE - 1, width), :]
                        )
                    )

        loop(body)

    for _ in range(STEPS):
        stage(u, w1, 0, 1.0 / 3.0)
        stage(w1, w2, 1, 0.5)
        stage(w2, u, 2, 1.0)

    cell = lax.broadcasted_iota(jnp.int32, (sub, LANES), 0)
    low = jnp.bitwise_and(cell, 3)
    kept = divides(cell, cut_ref[0, 3])
    near = jnp.where(jnp.bitwise_and(low, 1) == 1, -0.5, 0.0) * kept
    far = jnp.where(low == 2, -0.5, 0.0) * kept

    def lines(start):
        product = split_product(flat_rows(u, start), lane_surplus[...])
        for r in range(chunk):
            for h in range(tiles):
                w1[h, start + r, body_rows, :] = cut_rows(product, r, h)
                at = [w1[h, start + r, pl.ds(TILE + HALO + by, sub), :] for by in (-2, -1, 0, 1, 2)]
                w2[h, start + r, pl.ds(TILE, sub), :] = (
                    kept * at[2] + near * (at[1] + at[3]) + far * (at[0] + at[4])
                )

    loop(lines)

    pieces = len(order)
    depth = sub // pieces
    count = pieces.bit_length() - 1
    scales = {2: divides(jnp.int32(2), cut_ref[0, 0]), 1: divides(jnp.int32(1), cut_ref[0, 0])}
    for slot, q in enumerate(order):
        offset = pl.multiple_of(TILE + piece_at(q, count) * depth, TILE)
        out, index = out_refs[slot // out_refs[0].shape[0]], slot % out_refs[0].shape[0]
        for h in range(tiles):
            line = [w2[h, i, pl.ds(offset, depth), :] for i in range(total)]
            for i in range(total):
                value = line[i]
                if i % 4:
                    hop = 2 if i % 2 == 0 else 1
                    value = scales[hop] * (value - 0.5 * (line[i - hop] + line[(i + hop) % total]))
                out[index, i, :, pl.ds(h * LANES, LANES)] = value


def evolve(cutoffs, diffusion, courant, mats, parts, order):
    dom, arrays = len(parts[0]), len(parts)
    rows, lanes = parts[0][0].shape[0], parts[0][0].shape[2]
    sub = min(p[0].shape[1] for p in parts)
    if arrays == 1:
        sub -= 2 * HALO
    total = rows * dom
    width = sub + 2 * HALO
    pieces = len(order)
    kept = max(pieces // 2, 1)
    outs = [floats(kept, total, sub // pieces, lanes)] * min(pieces, 2)
    state = (lanes // LANES, total, width + 2 * TILE, LANES)
    chunk = min(16, total)
    flat = [p for part in parts for p in part]
    return pl.pallas_call(
        functools.partial(evolve_kernel, (dom, order, chunk, arrays)),
        out_shape=outs,
        in_specs=[SMEM] * 3 + [VMEM] * (3 + len(flat)),
        out_specs=[VMEM] * len(outs),
        scratch_shapes=[pltpu.VMEM(state, jnp.float32)] * 3,
        compiler_params=params(*flat, *outs, *[floats(*state)] * 3),
    )(cutoffs, diffusion, courant, *mats, *flat)


def rows_kernel(dom, scale, *refs):
    in_refs, out_refs = refs[:-2], refs[-2:]
    total = in_refs[0].shape[0]
    rows = total // dom
    place = lax.axis_index("dom")

    def row(i):
        value = in_refs[0][pl.ds(i, 1)]
        for ref in in_refs[1:]:
            value += ref[pl.ds(i, 1)]
        return value * scale

    for k in range(dom):
        first = (place ^ k) * rows
        out, slot = out_refs[k // (dom // 2)], k % (dom // 2)
        for r in range(rows + 1):
            i = first + r if r < rows else lax.rem(first + rows, total)
            out[slot, pl.ds(r, 1)] = row(i)


def rows_for(dom, scale, addends):
    total, depth, lanes = addends[0].shape
    outs = [floats(dom // 2, total // dom + 1, depth, lanes)] * 2
    return pl.pallas_call(
        functools.partial(rows_kernel, dom, scale),
        out_shape=outs,
        in_specs=[VMEM] * len(addends),
        out_specs=[VMEM] * 2,
        compiler_params=params(*addends, *outs),
    )(*addends)


def exchange_rows(keep, send, dom):
    sources = [0]
    keep, send = keep[:, None], send[:, None]
    bit = dom // 2
    while True:
        held = jnp.concatenate([keep, swapped(send, "dom", bit)], axis=1)
        sources = sources + [s | bit for s in sources]
        if bit == 1:
            return held[0], tuple(sources)
        bit //= 2
        keep, send = held[:bit], held[bit:]


def restore_kernel(plan, cut_ref, lane_restore, *refs):
    dom, groups = plan
    in_refs, out_ref, summed = refs[:-2], refs[-2], refs[-1]
    rows, lanes, length = out_ref.shape
    place = lax.axis_index("dom")
    block = length // dom
    for ref, (chain, count, slots, sources) in zip(in_refs, groups):
        depth = block // CHAINS >> count
        for s, q in enumerate(slots):
            piece = chain * (block // CHAINS) + piece_at(q, count) * depth
            for m, k in enumerate(sources):
                at = pl.multiple_of((place ^ k) * block + piece, TILE)
                summed[:, pl.ds(at, depth), :] = ref[s, m]

    cell = lax.broadcasted_iota(jnp.int32, (length, lanes), 0)
    low = jnp.bitwise_and(cell, 3)
    kept = divides(cell, cut_ref[0, 3])
    far = jnp.where(low == 2, 0.5, 0.0)
    near = jnp.where(jnp.bitwise_and(low, 1) == 1, 0.5, 0.0)

    def along_cells(v):
        v = kept * v
        v = v + far * (pltpu.roll(v, length - 2, 0) + pltpu.roll(v, 2, 0))
        v = v + near * (pltpu.roll(v, length - 1, 0) + pltpu.roll(v, 1, 0))
        high, low_part = halves(v)
        dims = (((1,), (1,)), ((), ()))
        dot = functools.partial(lax.dot_general, dimension_numbers=dims, preferred_element_type=jnp.float32)
        return dot(lane_restore[...], high) + dot(lane_restore[...], low_part)

    one = divides(jnp.int32(1), cut_ref[0, 0])
    two = divides(jnp.int32(2), cut_ref[0, 0])
    for r in range(0, rows, 4):
        first, last = summed[r], summed[r + 4]
        middle = two * summed[r + 2] + 0.5 * (first + last)
        out_ref[r] = along_cells(first)
        out_ref[r + 1] = along_cells(one * summed[r + 1] + 0.5 * (first + middle))
        out_ref[r + 2] = along_cells(middle)
        out_ref[r + 3] = along_cells(one * summed[r + 3] + 0.5 * (middle + last))


def restore(cutoffs, lane_restore, arrays, groups, dom, rows, lanes, length):
    out = floats(rows, lanes, length)
    return pl.pallas_call(
        functools.partial(restore_kernel, (dom, groups)),
        out_shape=out,
        in_specs=[SMEM, VMEM] + [VMEM] * len(arrays),
        out_specs=VMEM,
        scratch_shapes=[pltpu.VMEM((rows + 1, length, lanes), jnp.float32)],
        compiler_params=params(*arrays, out, floats(rows + 1, length, lanes)),
    )(cutoffs, lane_restore, *arrays)


def slot_order(count):
    order = [0]
    for i in reversed(range(count)):
        order = order + [q | 1 << i for q in order]
    return tuple(order)


def grid_sum(first, count, bits):
    state = list(first)
    for i in range(count - 1):
        added = state[0] + swapped_in_turn(state[1], i, count)
        half = added.shape[0] // 2
        state = [added[:half], added[half:]]
    addends = [state[0][0]]
    if count:
        addends.append(swapped_in_turn(state[1], count - 1, count)[0])
    for bit in bits[count:]:
        own = sum(addends[1:], addends[0])
        addends = [own, swapped(own, "grid", bit)]
    return addends


def shards(fields, cutoffs, weights, diffusion, courant):
    rows, second_len, third_len, length = fields.shape[1:]
    lanes = second_len * third_len
    dom, grids = lax.axis_size("dom"), lax.axis_size("grid")
    sub = length // dom // CHAINS
    bits = [1 << i for i in range(grids.bit_length() - 1)]
    count = max(min(len(bits) - 1, (sub // TILE).bit_length() - 1), 0)
    order = slot_order(count)

    sent = windows(fields.reshape(rows, lanes, length), dom)
    mats = tables(cutoffs, weights, diffusion, courant, second_len, third_len)
    parts = [[s[0]] + [swapped(s[k], "dom", k) for k in range(1, dom)] for s in sent]

    arrays, groups = [], []
    for c in range(CHAINS):
        first = evolve(cutoffs, diffusion, courant, mats[:3], parts[: c + 1][-2:], order)
        addends = grid_sum(first, count, bits)
        home, sources = exchange_rows(*rows_for(dom, 1.0 / grids, addends), dom)
        held, slots = home[None], [0]
        for i in reversed(range(count)):
            arrived = swapped_in_turn(held, i, count)
            new_slots = [q | 1 << i for q in slots]
            if i:
                held, slots = jnp.concatenate([held, arrived]), slots + new_slots
            else:
                arrays.append(arrived)
                groups.append((c, count, tuple(new_slots), sources))
        arrays.append(held)
        groups.append((c, count, tuple(slots), sources))
    out = restore(cutoffs, mats[3], arrays, tuple(groups), dom, rows, lanes, length)
    return out.reshape(1, rows, second_len, third_len, length)


def solution(mesh):
    in_specs = (P("grid", "dom", None, None, None), P("grid", None), P("grid"), P(), P())
    out_specs = P("grid", "dom", None, None, None)
    return jax.shard_map(shards, mesh=mesh, in_specs=in_specs, out_specs=out_specs, check_vma=False)
```

```python
import functools

import jax
import jax.numpy as jnp
from jax import lax
from jax.experimental import pallas as pl
from jax.experimental.pallas import tpu as pltpu
from jax.sharding import PartitionSpec as P


STEPS = 2
HALO = 8
TILE = 8
LANES = 128
GROUP = 16
EAGER = "ab"
CHAINS = 2

VMEM = pl.BlockSpec(memory_space=pltpu.VMEM)
SMEM = pl.BlockSpec(memory_space=pltpu.SMEM)
FAR = pl.BlockSpec(memory_space=pltpu.HBM)


def params(*arrays):
    held = sum(a.size * a.dtype.itemsize for a in arrays)
    return pltpu.CompilerParams(vmem_limit_bytes=min(2 * held + (4 << 20), 60 << 20))


def floats(*shape):
    return jax.ShapeDtypeStruct(shape, jnp.float32)


def swapped(x, axis, bit):
    size = lax.axis_size(axis)
    return lax.ppermute(x, axis, [(i, i ^ bit) for i in range(size)])


def turned(i, core, count):
    return (i + core) % count


def swapped_in_turn(x, i, count):
    grids, dom = lax.axis_size("grid"), lax.axis_size("dom")
    pairs = []
    for g in range(grids):
        for d in range(dom):
            pairs.append((g * dom + d, (g ^ 1 << turned(i, d & 1, count)) * dom + d))
    return lax.ppermute(x, ("grid", "dom"), pairs)


def halves(x):
    high = x.astype(jnp.bfloat16)
    return high, (x - high.astype(jnp.float32)).astype(jnp.bfloat16)


def split_product(x, m_high, m_low=None):
    high, low = halves(x)
    dot = functools.partial(jnp.dot, preferred_element_type=jnp.float32)
    total = dot(high, m_high) + dot(low, m_high)
    return total if m_low is None else total + dot(high, m_low)


def divides(place, cutoff):
    return (jnp.bitwise_and(place, jnp.left_shift(1, cutoff) - 1) == 0).astype(jnp.float32)


def piece_at(slot, count):
    place, core = lax.axis_index("grid"), jnp.bitwise_and(lax.axis_index("dom"), 1)
    piece = jnp.bitwise_and(place, (1 << count) - 1)
    for i in range(count):
        if slot >> i & 1:
            piece = piece ^ jnp.left_shift(1, lax.rem(i + core, count))
    return piece


def surplus_entry(source, target, length):
    low = jnp.bitwise_and(target, 3)
    hop = jnp.where(low == 0, 0, jnp.where(low == 2, 2, 1))
    gap = jnp.bitwise_and(source - target, length - 1)
    beside = (gap == hop).astype(jnp.float32) + (gap == jnp.bitwise_and(-hop, length - 1)).astype(jnp.float32)
    return (gap == 0).astype(jnp.float32) - jnp.where(hop > 0, 0.5, 0.0) * beside


def restore_entry(source, target, length):
    low = jnp.bitwise_and(target, 3)
    gap = jnp.bitwise_and(source - target, length - 1)

    def at(by):
        return (gap == by % length).astype(jnp.float32)

    one = 0.75 * at(-1) + 0.5 * at(1) + 0.25 * at(3)
    three = 0.75 * at(1) + 0.5 * at(-1) + 0.25 * at(-3)
    two = 0.5 * (at(-2) + at(2))
    beside = jnp.where(low == 0, 0.0, jnp.where(low == 2, two, jnp.where(low == 1, one, three)))
    return at(0) + beside


def tables_kernel(lens, cut_ref, weight_ref, diff_ref, cour_ref, rate_high, rate_low, surplus_ref, restore_ref):
    second_len, third_len = lens
    shape = surplus_ref.shape
    row, col = (lax.broadcasted_iota(jnp.int32, shape, d) for d in (0, 1))
    shift = third_len.bit_length() - 1
    s_row, s_col = jnp.right_shift(row, shift), jnp.right_shift(col, shift)
    t_row, t_col = jnp.bitwise_and(row, third_len - 1), jnp.bitwise_and(col, third_len - 1)
    s_gap = jnp.bitwise_and(s_row - s_col, second_len - 1)
    t_gap = jnp.bitwise_and(t_row - t_col, third_len - 1)

    def where(cond, value):
        return jnp.where(cond, value, 0.0)

    spread = diff_ref[0] + diff_ref[1] + diff_ref[2] + diff_ref[3]
    rate = where((s_gap == 0) & (t_gap == 0), -2.0 * spread)
    rate += where((s_gap == 1) & (t_gap == 0), diff_ref[1] - cour_ref[1])
    rate += where((s_gap == second_len - 1) & (t_gap == 0), diff_ref[1] + cour_ref[1])
    rate += where((t_gap == 1) & (s_gap == 0), diff_ref[2] - cour_ref[2])
    rate += where((t_gap == third_len - 1) & (s_gap == 0), diff_ref[2] + cour_ref[2])
    for which, part in enumerate((1.0 / 3.0, 0.5, 1.0)):
        rate_high[which], rate_low[which] = halves(rate * part)

    kept = divides(s_col, cut_ref[0, 1]) * divides(t_col, cut_ref[0, 2])
    entry = surplus_entry(s_row, s_col, second_len) * surplus_entry(t_row, t_col, third_len)
    surplus_ref[...] = (kept * weight_ref[0].astype(jnp.float32) * entry).astype(jnp.bfloat16)
    entry = restore_entry(s_col, s_row, second_len) * restore_entry(t_col, t_row, third_len)
    restore_ref[...] = (kept * entry).astype(jnp.bfloat16)


def tables(cutoffs, weights, diffusion, courant, second_len, third_len):
    lanes = second_len * third_len
    one = jax.ShapeDtypeStruct((lanes, lanes), jnp.bfloat16)
    three = jax.ShapeDtypeStruct((3, lanes, lanes), jnp.bfloat16)
    outs = [three, three, one, one]
    return pl.pallas_call(
        functools.partial(tables_kernel, (second_len, third_len)),
        out_shape=outs,
        in_specs=[SMEM] * 4,
        out_specs=[VMEM] * 4,
        compiler_params=params(*outs),
    )(cutoffs, weights, diffusion, courant)


def windows_kernel(dom, u_ref, *refs):
    out_refs, ext = refs[:-1], refs[-1]
    rows, _, length = u_ref.shape
    block = length // dom
    place = lax.axis_index("dom")
    for r in range(rows):
        turned_row = u_ref[r].T
        ext[r, pl.ds(HALO, length), :] = turned_row
        ext[r, pl.ds(0, HALO), :] = turned_row[length - HALO :]
        ext[r, pl.ds(HALO + length, HALO), :] = turned_row[:HALO]
    for k in range(dom):
        start = pl.multiple_of((place ^ k) * block, TILE)
        for c in range(CHAINS):
            out = out_refs[c * dom + k]
            out[...] = ext[:, pl.ds(start, out.shape[1]), :]
            start += out.shape[1]


def windows(u, dom):
    rows, lanes, length = u.shape
    sub = length // dom // CHAINS
    outs = [floats(rows, sub + 2 * HALO if c == 0 else sub, lanes) for c in range(CHAINS) for _ in range(dom)]
    ext = (rows, length + 2 * HALO, lanes)
    sent = pl.pallas_call(
        functools.partial(windows_kernel, dom),
        out_shape=outs,
        in_specs=[VMEM],
        out_specs=[VMEM] * len(outs),
        scratch_shapes=[pltpu.VMEM(ext, jnp.float32)],
        compiler_params=params(u, floats(*ext), *outs),
    )(u)
    return [sent[c * dom : (c + 1) * dom] for c in range(CHAINS)]


def evolve_kernel(plan, cut_ref, diff_ref, cour_ref, rate_high, rate_low, lane_surplus, *refs):
    dom, order, chunk, arrays = plan
    in_refs, refs = refs[: dom * arrays], refs[dom * arrays :]
    out_refs, (u, w1, w2) = refs[:-3], refs[-3:]
    rows = in_refs[0].shape[0]
    tiles, total, width, _ = u.shape
    width -= 3 * TILE
    sub = width - 2 * HALO
    place = lax.axis_index("dom")
    body_rows = pl.ds(TILE, width)
    for k in range(dom):
        at, need = TILE + width, width
        for a in reversed(range(arrays)):
            part = in_refs[a * dom + k]
            take = min(need, part.shape[1])
            at, need = at - take, need - take
            for h in range(tiles):
                u[h, pl.ds((place ^ k) * rows, rows), pl.ds(at, take), :] = part[
                    :, pl.ds(part.shape[1] - take, take), pl.ds(h * LANES, LANES)
                ]
    spare = jnp.zeros((tiles, total, TILE, LANES), jnp.float32)
    for ref in (u, w1, w2):
        ref[:, :, pl.ds(0, TILE), :] = spare
        ref[:, :, pl.ds(TILE + width, TILE), :] = spare

    def flat_rows(source, start):
        return jnp.concatenate(
            [
                jnp.concatenate([source[h, start + r, body_rows, :] for h in range(tiles)], axis=1)
                for r in range(chunk)
            ],
            axis=0,
        )

    def cut_rows(product, r, h):
        return product[r * width : (r + 1) * width, h * LANES : (h + 1) * LANES]

    def loop(body):
        group = min(GROUP, total)

        def rows_of(start):
            for c in range(0, group, chunk):
                body(start + c)

        if group == total:
            rows_of(0)
        else:
            lax.fori_loop(0, total // group, lambda g, carry: (rows_of(g * group), carry)[1], 0)

    def around(i):
        return i % total if isinstance(i, int) else lax.rem(i, total)

    def stage(source, target, which, part):
        first = [part * (diff_ref[d] - cour_ref[d]) for d in (0, 3)]
        second = [part * (diff_ref[d] + cour_ref[d]) for d in (0, 3)]

        def body(start):
            product = split_product(flat_rows(source, start), rate_high[which], rate_low[which])
            for r in range(chunk):
                i = start + r
                above = around(i + 1) if r + 1 == chunk else i + 1
                below = around(i + total - 1) if r == 0 else i - 1
                for h in range(tiles):
                    target[h, i, body_rows, :] = (
                        u[h, i, body_rows, :]
                        + cut_rows(product, r, h)
                        + (first[0] * source[h, above, body_rows, :] + second[0] * source[h, below, body_rows, :])
                        + (
                            first[1] * source[h, i, pl.ds(TILE + 1, width), :]
                            + second[1] * source[h, i, pl.ds(TILE - 1, width), :]
                        )
                    )

        loop(body)

    for _ in range(STEPS):
        stage(u, w1, 0, 1.0 / 3.0)
        stage(w1, w2, 1, 0.5)
        stage(w2, u, 2, 1.0)

    cell = lax.broadcasted_iota(jnp.int32, (sub, LANES), 0)
    low = jnp.bitwise_and(cell, 3)
    kept = divides(cell, cut_ref[0, 3])
    near = jnp.where(jnp.bitwise_and(low, 1) == 1, -0.5, 0.0) * kept
    far = jnp.where(low == 2, -0.5, 0.0) * kept

    def lines(start):
        product = split_product(flat_rows(u, start), lane_surplus[...])
        for r in range(chunk):
            for h in range(tiles):
                w1[h, start + r, body_rows, :] = cut_rows(product, r, h)
                at = [w1[h, start + r, pl.ds(TILE + HALO + by, sub), :] for by in (-2, -1, 0, 1, 2)]
                w2[h, start + r, pl.ds(TILE, sub), :] = (
                    kept * at[2] + near * (at[1] + at[3]) + far * (at[0] + at[4])
                )

    loop(lines)

    pieces = len(order)
    depth = sub // pieces
    count = pieces.bit_length() - 1
    scales = {2: divides(jnp.int32(2), cut_ref[0, 0]), 1: divides(jnp.int32(1), cut_ref[0, 0])}
    for slot, q in enumerate(order):
        offset = pl.multiple_of(TILE + piece_at(q, count) * depth, TILE)
        out, index = out_refs[slot // out_refs[0].shape[0]], slot % out_refs[0].shape[0]
        for h in range(tiles):
            line = [w2[h, i, pl.ds(offset, depth), :] for i in range(total)]
            for i in range(total):
                value = line[i]
                if i % 4:
                    hop = 2 if i % 2 == 0 else 1
                    value = scales[hop] * (value - 0.5 * (line[i - hop] + line[(i + hop) % total]))
                out[index, i, :, pl.ds(h * LANES, LANES)] = value


def evolve(cutoffs, diffusion, courant, mats, parts, order):
    dom, arrays = len(parts[0]), len(parts)
    rows, lanes = parts[0][0].shape[0], parts[0][0].shape[2]
    sub = min(p[0].shape[1] for p in parts)
    if arrays == 1:
        sub -= 2 * HALO
    total = rows * dom
    width = sub + 2 * HALO
    pieces = len(order)
    kept = max(pieces // 2, 1)
    outs = [floats(kept, total, sub // pieces, lanes)] * min(pieces, 2)
    state = (lanes // LANES, total, width + 3 * TILE, LANES)
    chunk = min(4, total)
    flat = [p for part in parts for p in part]
    return pl.pallas_call(
        functools.partial(evolve_kernel, (dom, order, chunk, arrays)),
        out_shape=outs,
        in_specs=[SMEM] * 3 + [VMEM] * (3 + len(flat)),
        out_specs=[VMEM] * len(outs),
        scratch_shapes=[pltpu.VMEM(state, jnp.float32)] * 3,
        compiler_params=params(*flat, *outs, *[floats(*state)] * 3),
    )(cutoffs, diffusion, courant, *mats, *flat)


def rows_kernel(dom, scale, *refs):
    in_refs, out_refs = refs[:-2], refs[-2:]
    total = in_refs[0].shape[0]
    rows = total // dom
    place = lax.axis_index("dom")

    def row(i):
        value = in_refs[0][pl.ds(i, 1)]
        for ref in in_refs[1:]:
            value += ref[pl.ds(i, 1)]
        return value * scale

    for k in range(dom):
        first = (place ^ k) * rows
        out, slot = out_refs[k // (dom // 2)], k % (dom // 2)
        for r in range(rows + 1):
            i = first + r if r < rows else lax.rem(first + rows, total)
            out[slot, pl.ds(r, 1)] = row(i)


def rows_for(dom, scale, addends):
    total, depth, lanes = addends[0].shape
    outs = [floats(dom // 2, total // dom + 1, depth, lanes)] * 2
    return pl.pallas_call(
        functools.partial(rows_kernel, dom, scale),
        out_shape=outs,
        in_specs=[VMEM] * len(addends),
        out_specs=[VMEM] * 2,
        compiler_params=params(*addends, *outs),
    )(*addends)


def exchange_rows(keep, send, dom):
    sources = [0]
    keep, send = keep[:, None], send[:, None]
    bit = dom // 2
    while True:
        held = jnp.concatenate([keep, swapped(send, "dom", bit)], axis=1)
        sources = sources + [s | bit for s in sources]
        if bit == 1:
            return held[0], tuple(sources)
        bit = bit // 2
        keep, send = held[:bit], held[bit:]


def restore_kernel(plan, cut_ref, lane_restore, *refs):
    dom, groups = plan
    in_refs, out_ref, (summed, lined, held, written) = refs[:-5], refs[-5], refs[-4:]
    rows, lanes, length = out_ref.shape
    tiles = lanes // LANES
    place = lax.axis_index("dom")
    block = length // dom
    for ref, (chain, count, slots, sources) in zip(in_refs, groups):
        depth = block // CHAINS >> count
        for s, q in enumerate(slots):
            piece = chain * (block // CHAINS) + piece_at(q, count) * depth
            for m, k in enumerate(sources):
                at = pl.multiple_of(TILE + (place ^ k) * block + piece, TILE)
                for h in range(tiles):
                    summed[h, :, pl.ds(at, depth), :] = ref[s, m, :, :, pl.ds(h * LANES, LANES)]
    summed[:, :, pl.ds(TILE + length, TILE), :] = summed[:, :, pl.ds(TILE, TILE), :]
    summed[:, :, pl.ds(0, TILE), :] = jnp.zeros((tiles, rows + 1, TILE, LANES), jnp.float32)
    lined[:, :, pl.ds(0, TILE), :] = jnp.zeros((tiles, rows, TILE, LANES), jnp.float32)

    cell = lax.broadcasted_iota(jnp.int32, (length, LANES), 0)
    low = jnp.bitwise_and(cell, 3)
    kept = divides(cell, cut_ref[0, 3])
    far = jnp.where(low == 2, 0.5, 0.0)
    near = jnp.where(jnp.bitwise_and(low, 1) == 1, 0.5, 0.0)
    one = divides(jnp.int32(1), cut_ref[0, 0])
    two = divides(jnp.int32(2), cut_ref[0, 0])

    def along_rows(target, scale, before, after):
        for h in range(tiles):
            summed[h, target] = scale * summed[h, target] + 0.5 * (summed[h, before] + summed[h, after])

    def along_cells(r):
        for h in range(tiles):
            at = [summed[h, r, pl.ds(TILE + by, length), :] for by in (-2, 0, 2)]
            lined[h, r, pl.ds(TILE, length), :] = kept * at[1] + far * (at[0] + at[2])
            lined[h, r, pl.ds(TILE + length, TILE), :] = summed[h, r, pl.ds(TILE, TILE), :]
        line = []
        for h in range(tiles):
            at = [lined[h, r, pl.ds(TILE + by, length), :] for by in (-1, 0, 1)]
            line.append(at[1] + near * (at[0] + at[2]))
        high, low_part = halves(jnp.concatenate(line, axis=1))
        dims = (((1,), (1,)), ((), ()))
        dot = functools.partial(lax.dot_general, dimension_numbers=dims, preferred_element_type=jnp.float32)
        held[r] = dot(lane_restore[...], high) + dot(lane_restore[...], low_part)

    writes = [pltpu.make_async_copy(held.at[r], out_ref.at[r], written.at[r]) for r in range(rows)]
    for r in range(0, rows, 4):
        along_rows(r + 2, two, r, r + 4)
        along_rows(r + 1, one, r, r + 2)
        along_rows(r + 3, one, r + 2, r + 4)
        for i in range(r, r + 4):
            along_cells(i)
            writes[i].start()
    for write in writes:
        write.wait()


def restore(cutoffs, lane_restore, arrays, groups, dom, rows, lanes, length):
    out = floats(rows, lanes, length)
    summed, lined = [(lanes // LANES, n, length + 2 * TILE, LANES) for n in (rows + 1, rows)]
    return pl.pallas_call(
        functools.partial(restore_kernel, (dom, groups)),
        out_shape=out,
        in_specs=[SMEM, VMEM] + [VMEM] * len(arrays),
        out_specs=FAR,
        scratch_shapes=[
            pltpu.VMEM(summed, jnp.float32),
            pltpu.VMEM(lined, jnp.float32),
            pltpu.VMEM(out.shape, jnp.float32),
            pltpu.SemaphoreType.DMA((rows,)),
        ],
        compiler_params=params(*arrays, out, floats(*summed), floats(*lined)),
    )(cutoffs, lane_restore, *arrays)


def slot_order(count):
    order = [0]
    for i in reversed(range(count)):
        order = order + [q | 1 << i for q in order]
    return tuple(order)


def grid_sum(first, count, bits):
    state = list(first)
    for i in range(count - 1):
        added = state[0] + swapped_in_turn(state[1], i, count)
        half = added.shape[0] // 2
        state = [added[:half], added[half:]]
    addends = [state[0][0]]
    if count:
        addends.append(swapped_in_turn(state[1], count - 1, count)[0])
    for i, bit in enumerate(bits[count:], count):
        own = sum(addends[1:], addends[0])
        addends = [own, swapped(own, "grid", bit)]
    return addends


def shards(fields, cutoffs, weights, diffusion, courant):
    rows, second_len, third_len, length = fields.shape[1:]
    lanes = second_len * third_len
    dom, grids = lax.axis_size("dom"), lax.axis_size("grid")
    sub = length // dom // CHAINS
    bits = [1 << i for i in range(grids.bit_length() - 1)]
    count = max(min(len(bits) - 1, (sub // TILE).bit_length() - 1), 0)
    order = slot_order(count)

    sent = windows(fields.reshape(rows, lanes, length), dom)
    mats = tables(cutoffs, weights, diffusion, courant, second_len, third_len)
    parts = []
    for chain, s in zip("ab", sent):
        moved = [swapped(s[k], "dom", k) for k in reversed(range(1, dom))]
        parts.append([s[0]] + moved[::-1])

    arrays, groups = [], []
    for c in range(CHAINS):
        chain = "ab"[c]
        first = evolve(cutoffs, diffusion, courant, mats[:3], parts[: c + 1][-2:], order)
        addends = grid_sum(first, count, bits)
        needed = rows_for(dom, 1.0 / grids, addends)
        home, sources = exchange_rows(*needed, dom)
        held = [((0,), home[None])]
        for i in reversed(range(count)):
            for slots, piece in list(held):
                arrived = swapped_in_turn(piece, i, count)
                held.append((tuple(q | 1 << i for q in slots), arrived))
            if i and chain not in EAGER:
                slots = sum((slots for slots, _ in held), ())
                held = [(slots, jnp.concatenate([piece for _, piece in held]))]
        for slots, piece in held:
            arrays.append(piece)
            groups.append((c, count, slots, sources))
    out = restore(cutoffs, mats[3], arrays, tuple(groups), dom, rows, lanes, length)
    return out.reshape(1, rows, second_len, third_len, length)


def solution(mesh):
    in_specs = (P("grid", "dom", None, None, None), P("grid", None), P("grid"), P(), P())
    out_specs = P("grid", "dom", None, None, None)

    return jax.shard_map(shards, mesh=mesh, in_specs=in_specs, out_specs=out_specs, check_vma=False)
```

```python
import functools

import jax
import jax.numpy as jnp
from jax import lax
from jax.experimental import pallas as pl
from jax.experimental.pallas import tpu as pltpu
from jax.sharding import PartitionSpec as P


STEPS = 2
HALO = 8
TILE = 8
LANES = 128
GROUP = 16
EAGER = "ab"
CHAINS = 2

VMEM = pl.BlockSpec(memory_space=pltpu.VMEM)
SMEM = pl.BlockSpec(memory_space=pltpu.SMEM)
FAR = pl.BlockSpec(memory_space=pltpu.HBM)


def params(*arrays):
    held = sum(a.size * a.dtype.itemsize for a in arrays)
    return pltpu.CompilerParams(vmem_limit_bytes=min(2 * held + (4 << 20), 60 << 20))


def floats(*shape):
    return jax.ShapeDtypeStruct(shape, jnp.float32)


def swapped(x, axis, bit):
    size = lax.axis_size(axis)
    return lax.ppermute(x, axis, [(i, i ^ bit) for i in range(size)])


def turned(i, core, count):
    return (i + core) % count


def swapped_in_turn(x, i, count):
    grids, dom = lax.axis_size("grid"), lax.axis_size("dom")
    pairs = []
    for g in range(grids):
        for d in range(dom):
            pairs.append((g * dom + d, (g ^ 1 << turned(i, d & 1, count)) * dom + d))
    return lax.ppermute(x, ("grid", "dom"), pairs)


def halves(x):
    high = x.astype(jnp.bfloat16)
    return high, (x - high.astype(jnp.float32)).astype(jnp.bfloat16)


def split_product(x, m_high, m_low=None):
    high, low = halves(x)
    dot = functools.partial(jnp.dot, preferred_element_type=jnp.float32)
    total = dot(high, m_high) + dot(low, m_high)
    return total if m_low is None else total + dot(high, m_low)


def divides(place, cutoff):
    return (jnp.bitwise_and(place, jnp.left_shift(1, cutoff) - 1) == 0).astype(jnp.float32)


def piece_at(slot, count):
    place, core = lax.axis_index("grid"), jnp.bitwise_and(lax.axis_index("dom"), 1)
    piece = jnp.bitwise_and(place, (1 << count) - 1)
    for i in range(count):
        if slot >> i & 1:
            piece = piece ^ jnp.left_shift(1, lax.rem(i + core, count))
    return piece


def surplus_entry(source, target, length):
    low = jnp.bitwise_and(target, 3)
    hop = jnp.where(low == 0, 0, jnp.where(low == 2, 2, 1))
    gap = jnp.bitwise_and(source - target, length - 1)
    beside = (gap == hop).astype(jnp.float32) + (gap == jnp.bitwise_and(-hop, length - 1)).astype(jnp.float32)
    return (gap == 0).astype(jnp.float32) - jnp.where(hop > 0, 0.5, 0.0) * beside


def restore_entry(source, target, length):
    low = jnp.bitwise_and(target, 3)
    gap = jnp.bitwise_and(source - target, length - 1)

    def at(by):
        return (gap == by % length).astype(jnp.float32)

    one = 0.75 * at(-1) + 0.5 * at(1) + 0.25 * at(3)
    three = 0.75 * at(1) + 0.5 * at(-1) + 0.25 * at(-3)
    two = 0.5 * (at(-2) + at(2))
    beside = jnp.where(low == 0, 0.0, jnp.where(low == 2, two, jnp.where(low == 1, one, three)))
    return at(0) + beside


def tables_kernel(lens, cut_ref, weight_ref, diff_ref, cour_ref, rate_high, rate_low, surplus_ref, restore_ref):
    second_len, third_len = lens
    shape = surplus_ref.shape
    row, col = (lax.broadcasted_iota(jnp.int32, shape, d) for d in (0, 1))
    shift = third_len.bit_length() - 1
    s_row, s_col = jnp.right_shift(row, shift), jnp.right_shift(col, shift)
    t_row, t_col = jnp.bitwise_and(row, third_len - 1), jnp.bitwise_and(col, third_len - 1)
    s_gap = jnp.bitwise_and(s_row - s_col, second_len - 1)
    t_gap = jnp.bitwise_and(t_row - t_col, third_len - 1)

    def where(cond, value):
        return jnp.where(cond, value, 0.0)

    spread = diff_ref[0] + diff_ref[1] + diff_ref[2] + diff_ref[3]
    rate = where((s_gap == 0) & (t_gap == 0), -2.0 * spread)
    rate += where((s_gap == 1) & (t_gap == 0), diff_ref[1] - cour_ref[1])
    rate += where((s_gap == second_len - 1) & (t_gap == 0), diff_ref[1] + cour_ref[1])
    rate += where((t_gap == 1) & (s_gap == 0), diff_ref[2] - cour_ref[2])
    rate += where((t_gap == third_len - 1) & (s_gap == 0), diff_ref[2] + cour_ref[2])
    for which, part in enumerate((1.0 / 3.0, 0.5, 1.0)):
        rate_high[which], rate_low[which] = halves(rate * part)

    kept = divides(s_col, cut_ref[0, 1]) * divides(t_col, cut_ref[0, 2])
    entry = surplus_entry(s_row, s_col, second_len) * surplus_entry(t_row, t_col, third_len)
    surplus_ref[...] = (kept * weight_ref[0].astype(jnp.float32) * entry).astype(jnp.bfloat16)
    entry = restore_entry(s_col, s_row, second_len) * restore_entry(t_col, t_row, third_len)
    restore_ref[...] = (kept * entry).astype(jnp.bfloat16)


def tables(cutoffs, weights, diffusion, courant, second_len, third_len):
    lanes = second_len * third_len
    one = jax.ShapeDtypeStruct((lanes, lanes), jnp.bfloat16)
    three = jax.ShapeDtypeStruct((3, lanes, lanes), jnp.bfloat16)
    outs = [three, three, one, one]
    return pl.pallas_call(
        functools.partial(tables_kernel, (second_len, third_len)),
        out_shape=outs,
        in_specs=[SMEM] * 4,
        out_specs=[VMEM] * 4,
        compiler_params=params(*outs),
    )(cutoffs, weights, diffusion, courant)


def windows_kernel(dom, u_ref, *refs):
    out_refs, ext = refs[:-1], refs[-1]
    rows, _, length = u_ref.shape
    block = length // dom
    place = lax.axis_index("dom")
    for r in range(rows):
        turned_row = u_ref[r].T
        ext[r, pl.ds(HALO, length), :] = turned_row
        ext[r, pl.ds(0, HALO), :] = turned_row[length - HALO :]
        ext[r, pl.ds(HALO + length, HALO), :] = turned_row[:HALO]
    for k in range(dom):
        start = pl.multiple_of((place ^ k) * block, TILE)
        for c in range(CHAINS):
            out = out_refs[c * dom + k]
            out[...] = ext[:, pl.ds(start, out.shape[1]), :]
            start += out.shape[1]


def windows(u, dom):
    rows, lanes, length = u.shape
    sub = length // dom // CHAINS
    outs = [floats(rows, sub + 2 * HALO if c == 0 else sub, lanes) for c in range(CHAINS) for _ in range(dom)]
    ext = (rows, length + 2 * HALO, lanes)
    sent = pl.pallas_call(
        functools.partial(windows_kernel, dom),
        out_shape=outs,
        in_specs=[VMEM],
        out_specs=[VMEM] * len(outs),
        scratch_shapes=[pltpu.VMEM(ext, jnp.float32)],
        compiler_params=params(u, floats(*ext), *outs),
    )(u)
    return [sent[c * dom : (c + 1) * dom] for c in range(CHAINS)]


def evolve_kernel(plan, cut_ref, diff_ref, cour_ref, rate_high, rate_low, lane_surplus, *refs):
    dom, order, chunk, arrays = plan
    in_refs, refs = refs[: dom * arrays], refs[dom * arrays :]
    out_refs, (u, w1, w2) = refs[:-3], refs[-3:]
    rows = in_refs[0].shape[0]
    tiles, total, width, _ = u.shape
    width -= 3 * TILE
    sub = width - 2 * HALO
    place = lax.axis_index("dom")
    body_rows = pl.ds(TILE, width)
    for k in range(dom):
        at, need = TILE + width, width
        for a in reversed(range(arrays)):
            part = in_refs[a * dom + k]
            take = min(need, part.shape[1])
            at, need = at - take, need - take
            for h in range(tiles):
                u[h, pl.ds((place ^ k) * rows, rows), pl.ds(at, take), :] = part[
                    :, pl.ds(part.shape[1] - take, take), pl.ds(h * LANES, LANES)
                ]
    spare = jnp.zeros((tiles, total, TILE, LANES), jnp.float32)
    for ref in (u, w1, w2):
        ref[:, :, pl.ds(0, TILE), :] = spare
        ref[:, :, pl.ds(TILE + width, TILE), :] = spare

    def flat_rows(source, start):
        return jnp.concatenate(
            [
                jnp.concatenate([source[h, start + r, body_rows, :] for h in range(tiles)], axis=1)
                for r in range(chunk)
            ],
            axis=0,
        )

    def cut_rows(product, r, h):
        return product[r * width : (r + 1) * width, h * LANES : (h + 1) * LANES]

    def loop(body):
        group = min(GROUP, total)

        def rows_of(start):
            for c in range(0, group, chunk):
                body(start + c)

        if group == total:
            rows_of(0)
        else:
            lax.fori_loop(0, total // group, lambda g, carry: (rows_of(g * group), carry)[1], 0)

    def around(i):
        return i % total if isinstance(i, int) else lax.rem(i, total)

    def stage(source, target, which, part):
        first = [part * (diff_ref[d] - cour_ref[d]) for d in (0, 3)]
        second = [part * (diff_ref[d] + cour_ref[d]) for d in (0, 3)]

        def body(start):
            product = split_product(flat_rows(source, start), rate_high[which], rate_low[which])
            for r in range(chunk):
                i = start + r
                above = around(i + 1) if r + 1 == chunk else i + 1
                below = around(i + total - 1) if r == 0 else i - 1
                for h in range(tiles):
                    target[h, i, body_rows, :] = (
                        u[h, i, body_rows, :]
                        + cut_rows(product, r, h)
                        + (first[0] * source[h, above, body_rows, :] + second[0] * source[h, below, body_rows, :])
                        + (
                            first[1] * source[h, i, pl.ds(TILE + 1, width), :]
                            + second[1] * source[h, i, pl.ds(TILE - 1, width), :]
                        )
                    )

        loop(body)

    for _ in range(STEPS):
        stage(u, w1, 0, 1.0 / 3.0)
        stage(w1, w2, 1, 0.5)
        stage(w2, u, 2, 1.0)

    cell = lax.broadcasted_iota(jnp.int32, (sub, LANES), 0)
    low = jnp.bitwise_and(cell, 3)
    kept = divides(cell, cut_ref[0, 3])
    near = jnp.where(jnp.bitwise_and(low, 1) == 1, -0.5, 0.0) * kept
    far = jnp.where(low == 2, -0.5, 0.0) * kept

    def lines(start):
        product = split_product(flat_rows(u, start), lane_surplus[...])
        for r in range(chunk):
            for h in range(tiles):
                w1[h, start + r, body_rows, :] = cut_rows(product, r, h)
                at = [w1[h, start + r, pl.ds(TILE + HALO + by, sub), :] for by in (-2, -1, 0, 1, 2)]
                w2[h, start + r, pl.ds(TILE, sub), :] = (
                    kept * at[2] + near * (at[1] + at[3]) + far * (at[0] + at[4])
                )

    loop(lines)

    pieces = len(order)
    depth = sub // pieces
    count = pieces.bit_length() - 1
    scales = {2: divides(jnp.int32(2), cut_ref[0, 0]), 1: divides(jnp.int32(1), cut_ref[0, 0])}
    for slot, q in enumerate(order):
        offset = pl.multiple_of(TILE + piece_at(q, count) * depth, TILE)
        out, index = out_refs[slot // out_refs[0].shape[0]], slot % out_refs[0].shape[0]
        for h in range(tiles):
            line = [w2[h, i, pl.ds(offset, depth), :] for i in range(total)]
            for i in range(total):
                value = line[i]
                if i % 4:
                    hop = 2 if i % 2 == 0 else 1
                    value = scales[hop] * (value - 0.5 * (line[i - hop] + line[(i + hop) % total]))
                out[index, i, :, pl.ds(h * LANES, LANES)] = value


def evolve(cutoffs, diffusion, courant, mats, parts, order):
    dom, arrays = len(parts[0]), len(parts)
    rows, lanes = parts[0][0].shape[0], parts[0][0].shape[2]
    sub = min(p[0].shape[1] for p in parts)
    if arrays == 1:
        sub -= 2 * HALO
    total = rows * dom
    width = sub + 2 * HALO
    pieces = len(order)
    kept = max(pieces // 2, 1)
    outs = [floats(kept, total, sub // pieces, lanes)] * min(pieces, 2)
    state = (lanes // LANES, total, width + 3 * TILE, LANES)
    chunk = min(4, total)
    flat = [p for part in parts for p in part]
    return pl.pallas_call(
        functools.partial(evolve_kernel, (dom, order, chunk, arrays)),
        out_shape=outs,
        in_specs=[SMEM] * 3 + [VMEM] * (3 + len(flat)),
        out_specs=[VMEM] * len(outs),
        scratch_shapes=[pltpu.VMEM(state, jnp.float32)] * 3,
        compiler_params=params(*flat, *outs, *[floats(*state)] * 3),
    )(cutoffs, diffusion, courant, *mats, *flat)


def rows_kernel(dom, scale, *refs):
    in_refs, out_refs = refs[:-dom], refs[-dom:]
    total = in_refs[0].shape[0]
    rows = total // dom
    place = lax.axis_index("dom")

    def row(i):
        value = in_refs[0][pl.ds(i, 1)]
        for ref in in_refs[1:]:
            value += ref[pl.ds(i, 1)]
        return value * scale

    for k in range(dom):
        first = (place ^ k) * rows
        for r in range(rows + 1):
            i = first + r if r < rows else lax.rem(first + rows, total)
            out_refs[k][0, pl.ds(r, 1)] = row(i)


def rows_for(dom, scale, addends):
    total, depth, lanes = addends[0].shape
    outs = [floats(1, total // dom + 1, depth, lanes)] * dom
    return pl.pallas_call(
        functools.partial(rows_kernel, dom, scale),
        out_shape=outs,
        in_specs=[VMEM] * len(addends),
        out_specs=[VMEM] * dom,
        compiler_params=params(*addends, *outs),
    )(*addends)


def exchange_rows(needed, dom):
    moved = [swapped(needed[k], "dom", k) for k in reversed(range(1, dom))]
    return jnp.concatenate([needed[0]] + moved[::-1]), tuple(range(dom))


def restore_kernel(plan, cut_ref, lane_restore, *refs):
    dom, groups = plan
    in_refs, out_ref, (summed, lined, held, written) = refs[:-5], refs[-5], refs[-4:]
    rows, lanes, length = out_ref.shape
    tiles = lanes // LANES
    place = lax.axis_index("dom")
    block = length // dom
    for ref, (chain, count, slots, sources) in zip(in_refs, groups):
        depth = block // CHAINS >> count
        for s, q in enumerate(slots):
            piece = chain * (block // CHAINS) + piece_at(q, count) * depth
            for m, k in enumerate(sources):
                at = pl.multiple_of(TILE + (place ^ k) * block + piece, TILE)
                for h in range(tiles):
                    summed[h, :, pl.ds(at, depth), :] = ref[s, m, :, :, pl.ds(h * LANES, LANES)]
    summed[:, :, pl.ds(TILE + length, TILE), :] = summed[:, :, pl.ds(TILE, TILE), :]
    summed[:, :, pl.ds(0, TILE), :] = jnp.zeros((tiles, rows + 1, TILE, LANES), jnp.float32)
    lined[:, :, pl.ds(0, TILE), :] = jnp.zeros((tiles, rows, TILE, LANES), jnp.float32)

    cell = lax.broadcasted_iota(jnp.int32, (length, LANES), 0)
    low = jnp.bitwise_and(cell, 3)
    kept = divides(cell, cut_ref[0, 3])
    far = jnp.where(low == 2, 0.5, 0.0)
    near = jnp.where(jnp.bitwise_and(low, 1) == 1, 0.5, 0.0)
    one = divides(jnp.int32(1), cut_ref[0, 0])
    two = divides(jnp.int32(2), cut_ref[0, 0])

    def along_rows(target, scale, before, after):
        for h in range(tiles):
            summed[h, target] = scale * summed[h, target] + 0.5 * (summed[h, before] + summed[h, after])

    def along_cells(r):
        for h in range(tiles):
            at = [summed[h, r, pl.ds(TILE + by, length), :] for by in (-2, 0, 2)]
            lined[h, r, pl.ds(TILE, length), :] = kept * at[1] + far * (at[0] + at[2])
            lined[h, r, pl.ds(TILE + length, TILE), :] = summed[h, r, pl.ds(TILE, TILE), :]
        line = []
        for h in range(tiles):
            at = [lined[h, r, pl.ds(TILE + by, length), :] for by in (-1, 0, 1)]
            line.append(at[1] + near * (at[0] + at[2]))
        high, low_part = halves(jnp.concatenate(line, axis=1))
        dims = (((1,), (1,)), ((), ()))
        dot = functools.partial(lax.dot_general, dimension_numbers=dims, preferred_element_type=jnp.float32)
        held[r] = dot(lane_restore[...], high) + dot(lane_restore[...], low_part)

    writes = [pltpu.make_async_copy(held.at[r], out_ref.at[r], written.at[r]) for r in range(rows)]
    for r in range(0, rows, 4):
        along_rows(r + 2, two, r, r + 4)
        along_rows(r + 1, one, r, r + 2)
        along_rows(r + 3, one, r + 2, r + 4)
        for i in range(r, r + 4):
            along_cells(i)
            writes[i].start()
    for write in writes:
        write.wait()


def restore(cutoffs, lane_restore, arrays, groups, dom, rows, lanes, length):
    out = floats(rows, lanes, length)
    summed, lined = [(lanes // LANES, n, length + 2 * TILE, LANES) for n in (rows + 1, rows)]
    return pl.pallas_call(
        functools.partial(restore_kernel, (dom, groups)),
        out_shape=out,
        in_specs=[SMEM, VMEM] + [VMEM] * len(arrays),
        out_specs=FAR,
        scratch_shapes=[
            pltpu.VMEM(summed, jnp.float32),
            pltpu.VMEM(lined, jnp.float32),
            pltpu.VMEM(out.shape, jnp.float32),
            pltpu.SemaphoreType.DMA((rows,)),
        ],
        compiler_params=params(*arrays, out, floats(*summed), floats(*lined)),
    )(cutoffs, lane_restore, *arrays)


def slot_order(count):
    order = [0]
    for i in reversed(range(count)):
        order = order + [q | 1 << i for q in order]
    return tuple(order)


def grid_sum(first, count, bits):
    state = list(first)
    for i in range(count - 1):
        added = state[0] + swapped_in_turn(state[1], i, count)
        half = added.shape[0] // 2
        state = [added[:half], added[half:]]
    addends = [state[0][0]]
    if count:
        addends.append(swapped_in_turn(state[1], count - 1, count)[0])
    for i, bit in enumerate(bits[count:], count):
        own = sum(addends[1:], addends[0])
        addends = [own, swapped(own, "grid", bit)]
    return addends


def shards(fields, cutoffs, weights, diffusion, courant):
    rows, second_len, third_len, length = fields.shape[1:]
    lanes = second_len * third_len
    dom, grids = lax.axis_size("dom"), lax.axis_size("grid")
    sub = length // dom // CHAINS
    bits = [1 << i for i in range(grids.bit_length() - 1)]
    count = max(min(len(bits) - 1, (sub // TILE).bit_length() - 1), 0)
    order = slot_order(count)

    sent = windows(fields.reshape(rows, lanes, length), dom)
    mats = tables(cutoffs, weights, diffusion, courant, second_len, third_len)
    parts = []
    for chain, s in zip("ab", sent):
        moved = [swapped(s[k], "dom", k) for k in reversed(range(1, dom))]
        parts.append([s[0]] + moved[::-1])

    arrays, groups = [], []
    for c in range(CHAINS):
        chain = "ab"[c]
        first = evolve(cutoffs, diffusion, courant, mats[:3], parts[: c + 1][-2:], order)
        addends = grid_sum(first, count, bits)
        needed = rows_for(dom, 1.0 / grids, addends)
        home, sources = exchange_rows(needed, dom)
        held = [((0,), home[None])]
        for i in reversed(range(count)):
            for slots, piece in list(held):
                arrived = swapped_in_turn(piece, i, count)
                held.append((tuple(q | 1 << i for q in slots), arrived))
            if i and chain not in EAGER:
                slots = sum((slots for slots, _ in held), ())
                held = [(slots, jnp.concatenate([piece for _, piece in held]))]
        for slots, piece in held:
            arrays.append(piece)
            groups.append((c, count, slots, sources))
    out = restore(cutoffs, mats[3], arrays, tuple(groups), dom, rows, lanes, length)
    return out.reshape(1, rows, second_len, third_len, length)


def solution(mesh):
    in_specs = (P("grid", "dom", None, None, None), P("grid", None), P("grid"), P(), P())
    out_specs = P("grid", "dom", None, None, None)

    return jax.shard_map(shards, mesh=mesh, in_specs=in_specs, out_specs=out_specs, check_vma=False)
```

```python
import functools

import jax
import jax.numpy as jnp
from jax import lax
from jax.experimental import pallas as pl
from jax.experimental.pallas import tpu as pltpu
from jax.sharding import PartitionSpec as P


STEPS = 2
HALO = 8
TILE = 8
LANES = 128
GROUP = 16
SPLIT = "b"
CHAINS = 2

VMEM = pl.BlockSpec(memory_space=pltpu.VMEM)
SMEM = pl.BlockSpec(memory_space=pltpu.SMEM)
FAR = pl.BlockSpec(memory_space=pltpu.HBM)


def params(*arrays):
    held = sum(a.size * a.dtype.itemsize for a in arrays)
    return pltpu.CompilerParams(vmem_limit_bytes=min(2 * held + (4 << 20), 60 << 20))


def floats(*shape):
    return jax.ShapeDtypeStruct(shape, jnp.float32)


def swapped(x, axis, bit):
    size = lax.axis_size(axis)
    return lax.ppermute(x, axis, [(i, i ^ bit) for i in range(size)])


def turned(i, core, count):
    return (i + core) % count


def swapped_in_turn(x, i, count):
    grids, dom = lax.axis_size("grid"), lax.axis_size("dom")
    pairs = []
    for g in range(grids):
        for d in range(dom):
            pairs.append((g * dom + d, (g ^ 1 << turned(i, d & 1, count)) * dom + d))
    return lax.ppermute(x, ("grid", "dom"), pairs)


def halves(x):
    high = x.astype(jnp.bfloat16)
    return high, (x - high.astype(jnp.float32)).astype(jnp.bfloat16)


def split_product(x, m_high, m_low=None):
    high, low = halves(x)
    dot = functools.partial(jnp.dot, preferred_element_type=jnp.float32)
    total = dot(high, m_high) + dot(low, m_high)
    return total if m_low is None else total + dot(high, m_low)


def divides(place, cutoff):
    return (jnp.bitwise_and(place, jnp.left_shift(1, cutoff) - 1) == 0).astype(jnp.float32)


def piece_at(slot, count):
    place, core = lax.axis_index("grid"), jnp.bitwise_and(lax.axis_index("dom"), 1)
    piece = jnp.bitwise_and(place, (1 << count) - 1)
    for i in range(count):
        if slot >> i & 1:
            piece = piece ^ jnp.left_shift(1, lax.rem(i + core, count))
    return piece


def surplus_entry(source, target, length):
    low = jnp.bitwise_and(target, 3)
    hop = jnp.where(low == 0, 0, jnp.where(low == 2, 2, 1))
    gap = jnp.bitwise_and(source - target, length - 1)
    beside = (gap == hop).astype(jnp.float32) + (gap == jnp.bitwise_and(-hop, length - 1)).astype(jnp.float32)
    return (gap == 0).astype(jnp.float32) - jnp.where(hop > 0, 0.5, 0.0) * beside


def restore_entry(source, target, length):
    low = jnp.bitwise_and(target, 3)
    gap = jnp.bitwise_and(source - target, length - 1)

    def at(by):
        return (gap == by % length).astype(jnp.float32)

    one = 0.75 * at(-1) + 0.5 * at(1) + 0.25 * at(3)
    three = 0.75 * at(1) + 0.5 * at(-1) + 0.25 * at(-3)
    two = 0.5 * (at(-2) + at(2))
    beside = jnp.where(low == 0, 0.0, jnp.where(low == 2, two, jnp.where(low == 1, one, three)))
    return at(0) + beside


def tables_kernel(lens, cut_ref, weight_ref, diff_ref, cour_ref, rate_high, rate_low, surplus_ref, restore_ref):
    second_len, third_len = lens
    shape = surplus_ref.shape
    row, col = (lax.broadcasted_iota(jnp.int32, shape, d) for d in (0, 1))
    shift = third_len.bit_length() - 1
    s_row, s_col = jnp.right_shift(row, shift), jnp.right_shift(col, shift)
    t_row, t_col = jnp.bitwise_and(row, third_len - 1), jnp.bitwise_and(col, third_len - 1)
    s_gap = jnp.bitwise_and(s_row - s_col, second_len - 1)
    t_gap = jnp.bitwise_and(t_row - t_col, third_len - 1)

    def where(cond, value):
        return jnp.where(cond, value, 0.0)

    spread = diff_ref[0] + diff_ref[1] + diff_ref[2] + diff_ref[3]
    rate = where((s_gap == 0) & (t_gap == 0), -2.0 * spread)
    rate += where((s_gap == 1) & (t_gap == 0), diff_ref[1] - cour_ref[1])
    rate += where((s_gap == second_len - 1) & (t_gap == 0), diff_ref[1] + cour_ref[1])
    rate += where((t_gap == 1) & (s_gap == 0), diff_ref[2] - cour_ref[2])
    rate += where((t_gap == third_len - 1) & (s_gap == 0), diff_ref[2] + cour_ref[2])
    for which, part in enumerate((1.0 / 3.0, 0.5, 1.0)):
        rate_high[which], rate_low[which] = halves(rate * part)

    kept = divides(s_col, cut_ref[0, 1]) * divides(t_col, cut_ref[0, 2])
    entry = surplus_entry(s_row, s_col, second_len) * surplus_entry(t_row, t_col, third_len)
    surplus_ref[...] = (kept * weight_ref[0].astype(jnp.float32) * entry).astype(jnp.bfloat16)
    entry = restore_entry(s_col, s_row, second_len) * restore_entry(t_col, t_row, third_len)
    restore_ref[...] = (kept * entry).astype(jnp.bfloat16)


def tables(cutoffs, weights, diffusion, courant, second_len, third_len):
    lanes = second_len * third_len
    one = jax.ShapeDtypeStruct((lanes, lanes), jnp.bfloat16)
    three = jax.ShapeDtypeStruct((3, lanes, lanes), jnp.bfloat16)
    outs = [three, three, one, one]
    return pl.pallas_call(
        functools.partial(tables_kernel, (second_len, third_len)),
        out_shape=outs,
        in_specs=[SMEM] * 4,
        out_specs=[VMEM] * 4,
        compiler_params=params(*outs),
    )(cutoffs, weights, diffusion, courant)


def windows_kernel(dom, u_ref, *refs):
    out_refs, ext = refs[:-1], refs[-1]
    rows, _, length = u_ref.shape
    block = length // dom
    place = lax.axis_index("dom")
    for r in range(rows):
        turned_row = u_ref[r].T
        ext[r, pl.ds(HALO, length), :] = turned_row
        ext[r, pl.ds(0, HALO), :] = turned_row[length - HALO :]
        ext[r, pl.ds(HALO + length, HALO), :] = turned_row[:HALO]
    for k in range(dom):
        start = pl.multiple_of((place ^ k) * block, TILE)
        for c in range(CHAINS):
            out = out_refs[c * dom + k]
            out[...] = ext[:, pl.ds(start, out.shape[1]), :]
            start += out.shape[1]


def windows(u, dom):
    rows, lanes, length = u.shape
    sub = length // dom // CHAINS
    outs = [floats(rows, sub + 2 * HALO if c == 0 else sub, lanes) for c in range(CHAINS) for _ in range(dom)]
    ext = (rows, length + 2 * HALO, lanes)
    sent = pl.pallas_call(
        functools.partial(windows_kernel, dom),
        out_shape=outs,
        in_specs=[VMEM],
        out_specs=[VMEM] * len(outs),
        scratch_shapes=[pltpu.VMEM(ext, jnp.float32)],
        compiler_params=params(u, floats(*ext), *outs),
    )(u)
    return [sent[c * dom : (c + 1) * dom] for c in range(CHAINS)]


def evolve_kernel(plan, cut_ref, diff_ref, cour_ref, rate_high, rate_low, lane_surplus, *refs):
    dom, order, chunk, arrays = plan
    in_refs, refs = refs[: dom * arrays], refs[dom * arrays :]
    out_refs, (u, w1, w2) = refs[:-3], refs[-3:]
    rows = in_refs[0].shape[0]
    tiles, total, width, _ = u.shape
    width -= 3 * TILE
    sub = width - 2 * HALO
    place = lax.axis_index("dom")
    body_rows = pl.ds(TILE, width)
    for k in range(dom):
        at, need = TILE + width, width
        for a in reversed(range(arrays)):
            part = in_refs[a * dom + k]
            take = min(need, part.shape[1])
            at, need = at - take, need - take
            for h in range(tiles):
                u[h, pl.ds((place ^ k) * rows, rows), pl.ds(at, take), :] = part[
                    :, pl.ds(part.shape[1] - take, take), pl.ds(h * LANES, LANES)
                ]
    spare = jnp.zeros((tiles, total, TILE, LANES), jnp.float32)
    for ref in (u, w1, w2):
        ref[:, :, pl.ds(0, TILE), :] = spare
        ref[:, :, pl.ds(TILE + width, TILE), :] = spare

    def flat_rows(source, start):
        return jnp.concatenate(
            [
                jnp.concatenate([source[h, start + r, body_rows, :] for h in range(tiles)], axis=1)
                for r in range(chunk)
            ],
            axis=0,
        )

    def cut_rows(product, r, h):
        return product[r * width : (r + 1) * width, h * LANES : (h + 1) * LANES]

    def loop(body):
        group = min(GROUP, total)

        def rows_of(start):
            for c in range(0, group, chunk):
                body(start + c)

        if group == total:
            rows_of(0)
        else:
            lax.fori_loop(0, total // group, lambda g, carry: (rows_of(g * group), carry)[1], 0)

    def around(i):
        return i % total if isinstance(i, int) else lax.rem(i, total)

    def stage(source, target, which, part):
        first = [part * (diff_ref[d] - cour_ref[d]) for d in (0, 3)]
        second = [part * (diff_ref[d] + cour_ref[d]) for d in (0, 3)]

        def body(start):
            product = split_product(flat_rows(source, start), rate_high[which], rate_low[which])
            for r in range(chunk):
                i = start + r
                above = around(i + 1) if r + 1 == chunk else i + 1
                below = around(i + total - 1) if r == 0 else i - 1
                for h in range(tiles):
                    target[h, i, body_rows, :] = (
                        u[h, i, body_rows, :]
                        + cut_rows(product, r, h)
                        + (first[0] * source[h, above, body_rows, :] + second[0] * source[h, below, body_rows, :])
                        + (
                            first[1] * source[h, i, pl.ds(TILE + 1, width), :]
                            + second[1] * source[h, i, pl.ds(TILE - 1, width), :]
                        )
                    )

        loop(body)

    for _ in range(STEPS):
        stage(u, w1, 0, 1.0 / 3.0)
        stage(w1, w2, 1, 0.5)
        stage(w2, u, 2, 1.0)

    cell = lax.broadcasted_iota(jnp.int32, (sub, LANES), 0)
    low = jnp.bitwise_and(cell, 3)
    kept = divides(cell, cut_ref[0, 3])
    near = jnp.where(jnp.bitwise_and(low, 1) == 1, -0.5, 0.0) * kept
    far = jnp.where(low == 2, -0.5, 0.0) * kept

    def lines(start):
        product = split_product(flat_rows(u, start), lane_surplus[...])
        for r in range(chunk):
            for h in range(tiles):
                w1[h, start + r, body_rows, :] = cut_rows(product, r, h)
                at = [w1[h, start + r, pl.ds(TILE + HALO + by, sub), :] for by in (-2, -1, 0, 1, 2)]
                w2[h, start + r, pl.ds(TILE, sub), :] = (
                    kept * at[2] + near * (at[1] + at[3]) + far * (at[0] + at[4])
                )

    loop(lines)

    pieces = len(order)
    depth = sub // pieces
    count = pieces.bit_length() - 1
    scales = {2: divides(jnp.int32(2), cut_ref[0, 0]), 1: divides(jnp.int32(1), cut_ref[0, 0])}
    for slot, q in enumerate(order):
        offset = pl.multiple_of(TILE + piece_at(q, count) * depth, TILE)
        out, index = out_refs[slot // out_refs[0].shape[0]], slot % out_refs[0].shape[0]
        for h in range(tiles):
            line = [w2[h, i, pl.ds(offset, depth), :] for i in range(total)]
            for i in range(total):
                value = line[i]
                if i % 4:
                    hop = 2 if i % 2 == 0 else 1
                    value = scales[hop] * (value - 0.5 * (line[i - hop] + line[(i + hop) % total]))
                out[index, i, :, pl.ds(h * LANES, LANES)] = value


def evolve(cutoffs, diffusion, courant, mats, parts, order):
    dom, arrays = len(parts[0]), len(parts)
    rows, lanes = parts[0][0].shape[0], parts[0][0].shape[2]
    sub = min(p[0].shape[1] for p in parts)
    if arrays == 1:
        sub -= 2 * HALO
    total = rows * dom
    width = sub + 2 * HALO
    pieces = len(order)
    kept = max(pieces // 2, 1)
    outs = [floats(kept, total, sub // pieces, lanes)] * min(pieces, 2)
    state = (lanes // LANES, total, width + 3 * TILE, LANES)
    chunk = min(4, total)
    flat = [p for part in parts for p in part]
    return pl.pallas_call(
        functools.partial(evolve_kernel, (dom, order, chunk, arrays)),
        out_shape=outs,
        in_specs=[SMEM] * 3 + [VMEM] * (3 + len(flat)),
        out_specs=[VMEM] * len(outs),
        scratch_shapes=[pltpu.VMEM(state, jnp.float32)] * 3,
        compiler_params=params(*flat, *outs, *[floats(*state)] * 3),
    )(cutoffs, diffusion, courant, *mats, *flat)


def rows_kernel(dom, scale, *refs):
    in_refs, out_refs = refs[:-dom], refs[-dom:]
    total = in_refs[0].shape[0]
    rows = total // dom
    place = lax.axis_index("dom")

    def row(i):
        value = in_refs[0][pl.ds(i, 1)]
        for ref in in_refs[1:]:
            value += ref[pl.ds(i, 1)]
        return value * scale

    for k in range(dom):
        first = (place ^ k) * rows
        for r in range(rows + 1):
            i = first + r if r < rows else lax.rem(first + rows, total)
            out_refs[k][0, pl.ds(r, 1)] = row(i)


def rows_for(dom, scale, addends):
    total, depth, lanes = addends[0].shape
    outs = [floats(1, total // dom + 1, depth, lanes)] * dom
    return pl.pallas_call(
        functools.partial(rows_kernel, dom, scale),
        out_shape=outs,
        in_specs=[VMEM] * len(addends),
        out_specs=[VMEM] * dom,
        compiler_params=params(*addends, *outs),
    )(*addends)


def exchange_rows(needed, dom):
    moved = [swapped(needed[k], "dom", k) for k in reversed(range(1, dom))]
    return [needed[0]] + moved[::-1]


def restore_kernel(plan, cut_ref, lane_restore, *refs):
    dom, groups = plan
    in_refs, out_ref, (summed, lined, held, written) = refs[:-5], refs[-5], refs[-4:]
    rows, lanes, length = out_ref.shape
    tiles = lanes // LANES
    place = lax.axis_index("dom")
    block = length // dom
    for ref, (chain, count, slots, sources) in zip(in_refs, groups):
        depth = block // CHAINS >> count
        for s, q in enumerate(slots):
            piece = chain * (block // CHAINS) + piece_at(q, count) * depth
            for m, k in enumerate(sources):
                at = pl.multiple_of(TILE + (place ^ k) * block + piece, TILE)
                for h in range(tiles):
                    summed[h, :, pl.ds(at, depth), :] = ref[s, m, :, :, pl.ds(h * LANES, LANES)]
    summed[:, :, pl.ds(TILE + length, TILE), :] = summed[:, :, pl.ds(TILE, TILE), :]
    summed[:, :, pl.ds(0, TILE), :] = jnp.zeros((tiles, rows + 1, TILE, LANES), jnp.float32)
    lined[:, :, pl.ds(0, TILE), :] = jnp.zeros((tiles, rows, TILE, LANES), jnp.float32)

    cell = lax.broadcasted_iota(jnp.int32, (length, LANES), 0)
    low = jnp.bitwise_and(cell, 3)
    kept = divides(cell, cut_ref[0, 3])
    far = jnp.where(low == 2, 0.5, 0.0)
    near = jnp.where(jnp.bitwise_and(low, 1) == 1, 0.5, 0.0)
    one = divides(jnp.int32(1), cut_ref[0, 0])
    two = divides(jnp.int32(2), cut_ref[0, 0])

    def along_rows(target, scale, before, after):
        for h in range(tiles):
            summed[h, target] = scale * summed[h, target] + 0.5 * (summed[h, before] + summed[h, after])

    def along_cells(r):
        for h in range(tiles):
            at = [summed[h, r, pl.ds(TILE + by, length), :] for by in (-2, 0, 2)]
            lined[h, r, pl.ds(TILE, length), :] = kept * at[1] + far * (at[0] + at[2])
            lined[h, r, pl.ds(TILE + length, TILE), :] = summed[h, r, pl.ds(TILE, TILE), :]
        line = []
        for h in range(tiles):
            at = [lined[h, r, pl.ds(TILE + by, length), :] for by in (-1, 0, 1)]
            line.append(at[1] + near * (at[0] + at[2]))
        high, low_part = halves(jnp.concatenate(line, axis=1))
        dims = (((1,), (1,)), ((), ()))
        dot = functools.partial(lax.dot_general, dimension_numbers=dims, preferred_element_type=jnp.float32)
        held[r] = dot(lane_restore[...], high) + dot(lane_restore[...], low_part)

    writes = [pltpu.make_async_copy(held.at[r], out_ref.at[r], written.at[r]) for r in range(rows)]
    for r in range(0, rows, 4):
        along_rows(r + 2, two, r, r + 4)
        along_rows(r + 1, one, r, r + 2)
        along_rows(r + 3, one, r + 2, r + 4)
        for i in range(r, r + 4):
            along_cells(i)
            writes[i].start()
    for write in writes:
        write.wait()


def restore(cutoffs, lane_restore, arrays, groups, dom, rows, lanes, length):
    out = floats(rows, lanes, length)
    summed, lined = [(lanes // LANES, n, length + 2 * TILE, LANES) for n in (rows + 1, rows)]
    return pl.pallas_call(
        functools.partial(restore_kernel, (dom, groups)),
        out_shape=out,
        in_specs=[SMEM, VMEM] + [VMEM] * len(arrays),
        out_specs=FAR,
        scratch_shapes=[
            pltpu.VMEM(summed, jnp.float32),
            pltpu.VMEM(lined, jnp.float32),
            pltpu.VMEM(out.shape, jnp.float32),
            pltpu.SemaphoreType.DMA((rows,)),
        ],
        compiler_params=params(*arrays, out, floats(*summed), floats(*lined)),
    )(cutoffs, lane_restore, *arrays)


def slot_order(count):
    order = [0]
    for i in reversed(range(count)):
        order = order + [q | 1 << i for q in order]
    return tuple(order)


def grid_sum(first, count, bits):
    state = list(first)
    for i in range(count - 1):
        added = state[0] + swapped_in_turn(state[1], i, count)
        half = added.shape[0] // 2
        state = [added[:half], added[half:]]
    addends = [state[0][0]]
    if count:
        addends.append(swapped_in_turn(state[1], count - 1, count)[0])
    for i, bit in enumerate(bits[count:], count):
        own = sum(addends[1:], addends[0])
        addends = [own, swapped(own, "grid", bit)]
    return addends


def shards(fields, cutoffs, weights, diffusion, courant):
    rows, second_len, third_len, length = fields.shape[1:]
    lanes = second_len * third_len
    dom, grids = lax.axis_size("dom"), lax.axis_size("grid")
    sub = length // dom // CHAINS
    bits = [1 << i for i in range(grids.bit_length() - 1)]
    count = max(min(len(bits) - 1, (sub // TILE).bit_length() - 1), 0)
    order = slot_order(count)

    sent = windows(fields.reshape(rows, lanes, length), dom)
    mats = tables(cutoffs, weights, diffusion, courant, second_len, third_len)
    parts = []
    for chain, s in zip("ab", sent):
        moved = [swapped(s[k], "dom", k) for k in reversed(range(1, dom))]
        parts.append([s[0]] + moved[::-1])

    arrays, groups = [], []
    for c in range(CHAINS):
        chain = "ab"[c]
        first = evolve(cutoffs, diffusion, courant, mats[:3], parts[: c + 1][-2:], order)
        addends = grid_sum(first, count, bits)
        needed = rows_for(dom, 1.0 / grids, addends)
        home, sources = exchange_rows(needed, dom), tuple(range(dom))
        parts_home = [(home, sources)]
        if chain in SPLIT:
            half = len(sources) // 2
            parts_home = [(home[:half], sources[:half]), (home[half:], sources[half:])]
        for some, places in parts_home:
            held = [((0,), jnp.concatenate(some)[None])]
            for i in reversed(range(count)):
                for slots, piece in list(held):
                    arrived = swapped_in_turn(piece, i, count)
                    held.append((tuple(q | 1 << i for q in slots), arrived))
            for slots, piece in held:
                arrays.append(piece)
                groups.append((c, count, slots, places))
    out = restore(cutoffs, mats[3], arrays, tuple(groups), dom, rows, lanes, length)
    return out.reshape(1, rows, second_len, third_len, length)


def solution(mesh):
    in_specs = (P("grid", "dom", None, None, None), P("grid", None), P("grid"), P(), P())
    out_specs = P("grid", "dom", None, None, None)

    return jax.shard_map(shards, mesh=mesh, in_specs=in_specs, out_specs=out_specs, check_vma=False)
```
